8 devices in a mesh: dp: 1 (over z), pp: 8 (over y, x, core).
Axes of the slice: x: 2, y: 2, z: 1, core: 2. Of those that a mesh axis runs over, the one named last changes fastest.
Arguments:
- x_in: bfloat16 [8, 1, 128, 1024], P(('dp', 'pp'))
- dy_out: bfloat16 [8, 1, 128, 1024], P(('dp', 'pp'))
- w_qkv: bfloat16 [8, 2, 1, 1024, 3, 16, 64], P('pp')
- w_attn: bfloat16 [8, 2, 1, 16, 64, 1024], P('pp')
- w_fc: bfloat16 [8, 2, 1, 1024, 4096], P('pp')
- w_proj: bfloat16 [8, 2, 1, 4096, 1024], P('pp')
- b_qkv: bfloat16 [8, 2, 1, 3, 16, 64], P('pp')
- b_fc: bfloat16 [8, 2, 1, 4096], P('pp')
- vec_d: bfloat16 [8, 2, 1, 6, 1024], P('pp')
Outputs:
- output 1: bfloat16 [8, 1, 128, 1024], P(('dp', 'pp'))
- output 2: bfloat16 [8, 1, 128, 1024], P(('dp', 'pp'))
- output 3: float32 [8, 2, 1, 1024, 3, 16, 64], P(('dp', 'pp'))
- output 4: float32 [8, 2, 1, 16, 64, 1024], P(('dp', 'pp'))
- output 5: float32 [8, 2, 1, 1024, 4096], P(('dp', 'pp'))
- output 6: float32 [8, 2, 1, 4096, 1024], P(('dp', 'pp'))
- output 7: float32 [8, 2, 1, 3, 16, 64], P(('dp', 'pp'))
- output 8: float32 [8, 2, 1, 4096], P(('dp', 'pp'))
- output 9: float32 [8, 2, 1, 6, 1024], P(('dp', 'pp'))
All inputs are finite; a program needn't handle non-finite values.
Results may differ from the reference program's by a relative error of at most 0.02.
Values are sent between devices in bfloat16 or wider.
A program may use at most 1 GiB of HBM per device.

```python
import jax
import jax.numpy as jnp
from jax import lax

STAGES = 8
MICRO = 8
LPS = 1
BATCH = 1
SEQ = 128
DM = 1024
HEADS = 16
FF = 4096
HEAD = DM // HEADS
LAYERS = STAGES * LPS
EPSILON = 1e-5


def with_second_copy(stage_major):
    return jnp.stack([stage_major, stage_major[::-1]], axis=1).astype(jnp.bfloat16)


def setup_inputs(seed: int = 0, part: int = 0) -> dict:
    root_key = jax.random.key(seed)
    data_keys = jax.random.split(jax.random.fold_in(root_key, part), 2)
    w_keys = jax.random.split(jax.random.key(seed + 7919), 7)
    res_scale = (2.0 * LAYERS) ** -0.5
    act_shape = (MICRO, BATCH, SEQ, DM)
    x_in = jax.random.normal(data_keys[0], act_shape, jnp.float32).astype(jnp.bfloat16)
    dy_out = jax.random.normal(data_keys[1], act_shape, jnp.float32).astype(jnp.bfloat16)
    w_qkv = with_second_copy(jax.random.normal(w_keys[0], (STAGES, LPS, DM, 3, HEADS, HEAD), jnp.float32) * DM ** -0.5)
    w_attn = with_second_copy(jax.random.normal(w_keys[1], (STAGES, LPS, HEADS, HEAD, DM), jnp.float32) * (DM ** -0.5 * res_scale))
    w_fc = with_second_copy(jax.random.normal(w_keys[2], (STAGES, LPS, DM, FF), jnp.float32) * DM ** -0.5)
    w_proj = with_second_copy(jax.random.normal(w_keys[3], (STAGES, LPS, FF, DM), jnp.float32) * (FF ** -0.5 * res_scale))
    b_qkv = with_second_copy(0.3 * jax.random.normal(w_keys[4], (STAGES, LPS, 3, HEADS, HEAD), jnp.float32))
    b_fc = with_second_copy(0.3 * jax.random.normal(w_keys[5], (STAGES, LPS, FF), jnp.float32))
    row_scale = jnp.array([0.2, 0.2, 0.5 * res_scale, 0.2, 0.2, 0.5 * res_scale], jnp.float32)
    row_shift = jnp.array([1.0, 0.0, 0.0, 1.0, 0.0, 0.0], jnp.float32)
    vec_rows = jax.random.normal(w_keys[6], (STAGES, LPS, 6, DM), jnp.float32)
    vec_d = with_second_copy(vec_rows * row_scale[:, None] + row_shift[:, None])
    return {'x_in': x_in, 'dy_out': dy_out, 'w_qkv': w_qkv, 'w_attn': w_attn, 'w_fc': w_fc, 'w_proj': w_proj, 'b_qkv': b_qkv, 'b_fc': b_fc, 'vec_d': vec_d}


def layer_norm(rows_in, ln_gain, ln_shift):
    rows_f32 = rows_in.astype(jnp.float32)
    row_mean = jnp.mean(rows_f32, axis=-1, keepdims=True)
    centered = rows_f32 - row_mean
    row_var = jnp.mean(centered * centered, axis=-1, keepdims=True)
    scaled = centered * lax.rsqrt(row_var + EPSILON)
    return (scaled * ln_gain.astype(jnp.float32) + ln_shift.astype(jnp.float32)).astype(jnp.bfloat16)


def gpt_layer(hidden_in, layer_w):
    w_qkv, w_attn, w_fc, w_proj, b_qkv, b_fc, vec_d = layer_w
    n_batch, seq_len, d_model = hidden_in.shape
    n_heads, head_dim = w_qkv.shape[-2], w_qkv.shape[-1]
    tokens = n_batch * seq_len
    flat_rows = hidden_in.reshape(tokens, d_model)
    normed = layer_norm(flat_rows, vec_d[0], vec_d[1])
    qkv_proj = jnp.dot(normed, w_qkv.reshape(d_model, 3 * d_model), preferred_element_type=jnp.float32)
    qkv_proj = (qkv_proj + b_qkv.reshape(3 * d_model).astype(jnp.float32)).astype(jnp.bfloat16)
    qkv_proj = qkv_proj.reshape(n_batch, seq_len, 3, n_heads, head_dim)
    query_heads = qkv_proj[:, :, 0].astype(jnp.float32)
    key_heads = qkv_proj[:, :, 1].astype(jnp.float32)
    value_heads = qkv_proj[:, :, 2].astype(jnp.float32)
    scores = jnp.einsum('bqhe,bkhe->bhqk', query_heads, key_heads) * (head_dim ** -0.5)
    causal = jnp.arange(seq_len)[:, None] >= jnp.arange(seq_len)[None, :]
    scores = jnp.where(causal, scores, -1e30)
    attn_probs = jax.nn.softmax(scores, axis=-1).astype(jnp.bfloat16)
    mixed_heads = jnp.einsum('bhqk,bkhe->bqhe', attn_probs.astype(jnp.float32), value_heads).astype(jnp.bfloat16)
    attn_out = jnp.dot(mixed_heads.reshape(tokens, d_model), w_attn.reshape(d_model, d_model), preferred_element_type=jnp.float32)
    residual = (flat_rows.astype(jnp.float32) + attn_out + vec_d[2].astype(jnp.float32)).astype(jnp.bfloat16)
    normed_two = layer_norm(residual, vec_d[3], vec_d[4])
    hidden = jnp.dot(normed_two, w_fc, preferred_element_type=jnp.float32) + b_fc.astype(jnp.float32)
    hidden = jax.nn.gelu(hidden, approximate=True).astype(jnp.bfloat16)
    mlp_out = jnp.dot(hidden, w_proj, preferred_element_type=jnp.float32) + vec_d[5].astype(jnp.float32)
    return (residual.astype(jnp.float32) + mlp_out).astype(jnp.bfloat16).reshape(n_batch, seq_len, d_model)


def stack_forward(hidden_in, layer_ws):
    def scan_body(carry, layer_w):
        return gpt_layer(carry, layer_w), None
    out_h, _ = lax.scan(scan_body, hidden_in, layer_ws)
    return out_h


def copy_pass(x_part, dy_part, layer_ws):
    grad_zero = tuple(jnp.zeros(t.shape, jnp.float32) for t in layer_ws)
    def scan_body(grad_acc, mb_pair):
        x_mb, dy_mb = mb_pair
        y_mb, pull_back = jax.vjp(stack_forward, x_mb, layer_ws)
        dx_mb, dw_mb = pull_back(dy_mb)
        grad_acc = tuple(a + g.astype(jnp.float32) for a, g in zip(grad_acc, dw_mb))
        return grad_acc, (y_mb, dx_mb)
    grad_acc, (y_half, dx_half) = lax.scan(scan_body, grad_zero, (x_part, dy_part))
    return y_half, dx_half, grad_acc


def reference(x_in, dy_out, w_qkv, w_attn, w_fc, w_proj, b_qkv, b_fc, vec_d):
    params = (w_qkv, w_attn, w_fc, w_proj, b_qkv, b_fc, vec_d)
    half_micro = MICRO // 2
    down_ws = tuple(t[:, 0].reshape((LAYERS,) + t.shape[3:]) for t in params)
    up_ws = tuple(t[::-1, 1].reshape((LAYERS,) + t.shape[3:]) for t in params)
    y_down, dx_down, g_down = copy_pass(x_in[:half_micro], dy_out[:half_micro], down_ws)
    y_up, dx_up, g_up = copy_pass(x_in[half_micro:], dy_out[half_micro:], up_ws)
    y_out = jnp.concatenate([y_down, y_up], axis=0)
    dx_in = jnp.concatenate([dx_down, dx_up], axis=0)
    grads = []
    for orig, part_down, part_up in zip(params, g_down, g_up):
        total = (part_down + part_up).reshape((STAGES, LPS) + orig.shape[3:])
        grads.append(jnp.stack([total, total[::-1]], axis=1))
    return (y_out, dx_in, grads[0], grads[1], grads[2], grads[3], grads[4], grads[5], grads[6])
```

```python
import jax
import jax.numpy as jnp
from jax import lax
from jax.experimental import pallas as pl
from jax.experimental.pallas import tpu as pltpu
from jax.sharding import PartitionSpec as P

EPSILON = 1e-5
SEQ = 128
DM = 1024
FF = 4096
MICRO = 8
OWN = MICRO // 2
PAIR = 2
PAIRS = MICRO // PAIR
ROWS = PAIR * SEQ
HV, DV, OUT, YO = 0, 2 * MICRO, 4 * MICRO, 6 * MICRO
N_SLOTS = 6 * MICRO + OWN
FWD, BWD = 0, 1
N_TASKS = 24
ORDER = (
    (0x56128398a418820, 0xb5250f3ddc6b34b),
    (0x5a927418a418820, 0xb5250f71eed3598),
    (0x619655112340820, 0xb53d2e434f761a7),
    (0x6958458d4248500, 0xb7a9c96a1879dc6),
)
GELU_C = 0.7978845608028654
GELU_CA = GELU_C * 0.044715
NEG = -1e30
MESH = pl.DeviceIdType.MESH
BF = jnp.bfloat16
F32 = jnp.float32


def dot_nn(a, b):
    return lax.dot_general(a, b, (((1,), (0,)), ((), ())), preferred_element_type=F32)


def dot_nt(a, b):
    return lax.dot_general(a, b, (((1,), (1,)), ((), ())), preferred_element_type=F32)


def dot_tn(a, b):
    return lax.dot_general(a, b, (((0,), (0,)), ((), ())), preferred_element_type=F32)


def normalize(rows_f32):
    mean = jnp.mean(rows_f32, axis=-1, keepdims=True)
    centered = rows_f32 - mean
    var = jnp.mean(centered * centered, axis=-1, keepdims=True)
    rstd = lax.rsqrt(var + EPSILON)
    return centered * rstd, rstd


def rounded(v):
    return v.astype(BF).astype(F32)


def block(j):
    return slice(j * DM, (j + 1) * DM)


def chain_kernel(x_hbm, dy_hbm, wq_hbm, wo_hbm, w1_hbm, w2_hbm, bq_in, bf_in, vec_in,
                 y_hbm, dx_hbm, a_hbm, t_hbm, o_hbm, h1_hbm, n2_hbm, z_hbm, u_hbm, p_hbm,
                 dz_hbm, dt_hbm, dh1_hbm, dh2_hbm, gbq_ref, gbf_ref, gvec_ref,
                 bq_ref, bf_ref, vec_ref, wbuf, w1buf, buf, a_v, t_v, o_v, h1_v, n2_v, z_v, u_v, p_v, dt_v, dh1_v, do_v,
                 wsem, w1sem, fsem, bsem, lsem, recv_x, recv_dy, send_x, send_dy,
                 send_f, recv_f, send_b, recv_b, send_y, recv_y, send_dx, recv_dx):
    me = lax.axis_index('pp')
    dp = lax.axis_index('dp')
    side = me // 4
    pos = me + side * (7 - 2 * me)

    def place(q):
        return (dp, q + side * (7 - 2 * q))

    def copy_of(leg):
        return leg + side - 2 * leg * side

    codes = []
    for s in range(N_TASKS):
        row = [jnp.int32((ORDER[q][s // 12] >> (5 * (s % 12))) % 32) for q in range(4)]
        codes.append(jnp.where(pos == 0, row[0], jnp.where(pos == 1, row[1], jnp.where(pos == 2, row[2], row[3]))))

    def code_at(s):
        c = codes[0]
        for k in range(1, N_TASKS):
            c = jnp.where(s == k, codes[k], c)
        return c

    def parts(code):
        return code // 16, (code // 8) % 2, code % 8

    barrier = pltpu.get_barrier_semaphore()
    for k in range(1, 8):
        pl.semaphore_signal(barrier, inc=1, device_id=(dp, lax.rem(me + k, 8)), device_id_type=MESH)
    pl.semaphore_wait(barrier, 7)

    def block_copy(b, leg):
        c = copy_of(leg)
        if b < 3:
            src = wq_hbm.at[c, pl.ds(b * DM, DM), :]
        elif b == 3:
            src = wo_hbm.at[c]
        else:
            src = w2_hbm.at[c, pl.ds((b - 4) * DM, DM), :]
        return pltpu.make_async_copy(src, wbuf.at[b], wsem.at[b])

    def w1_copy(j, leg):
        return pltpu.make_async_copy(w1_hbm.at[copy_of(leg), :, pl.ds(j * DM, DM)], w1buf.at[leg, j], w1sem.at[leg * 4 + j])

    first_leg = parts(codes[0])[1]
    for b in range(4):
        block_copy(b, first_leg).start()
    for j in range(4):
        w1_copy(j, first_leg).start()
        block_copy(4 + j, first_leg).start()
    for j in range(4):
        w1_copy(j, 1 - first_leg).start()

    def spread(src, base, send, recv, root_side):
        root = root_side * 7
        i = me + root_side * (7 - 2 * me)
        dst = buf.at[base + i]

        @pl.when(me == root)
        def _():
            pltpu.make_async_copy(src, dst, recv.at[i]).start()

        @pl.when(me != root)
        def _():
            pltpu.make_async_remote_copy(src_ref=src, dst_ref=dst, send_sem=send.at[root_side], recv_sem=recv.at[i],
                                         device_id=(dp, root), device_id_type=MESH).start()

    for src, base, send, recv in ((x_hbm, HV, send_x, recv_x), (dy_hbm, DV + MICRO, send_dy, recv_dy)):
        @pl.when(side == 0)
        def _():
            spread(src, base, send, recv, 0)
            spread(src, base, send, recv, 1)

        @pl.when(side == 1)
        def _():
            spread(src, base, send, recv, 1)
            spread(src, base, send, recv, 0)

    for c in range(2):
        bf_ref[c] = bf_in[c:c + 1, :].astype(F32)
        for n in range(6):
            vec_ref[c, n:n + 1, :] = vec_in[n, c:c + 1, :].astype(F32)
        for n in range(24):
            pair = bq_in[c, n // 8, 2 * (n % 8):2 * (n % 8) + 2, :].astype(F32)
            bq_ref[c, :, n * SEQ:(n + 1) * SEQ] = jnp.concatenate([pair[:1], pair[1:]], axis=1)
    gbq_ref[...] = jnp.zeros_like(gbq_ref)
    gbf_ref[...] = jnp.zeros_like(gbf_ref)
    gvec_ref[...] = jnp.zeros_like(gvec_ref)

    def upward(kind, leg):
        return leg if kind == BWD else 1 - leg

    def hop(kind, leg, i):
        k = leg * MICRO + i
        q = pos - 1 + 2 * upward(kind, leg)
        if kind == FWD:
            src, dst, send, recv = buf.at[OUT + k], buf.at[HV + k], send_f.at[k], recv_f.at[k]
        else:
            src, dst = buf.at[pl.ds(OUT + k, PAIR)], buf.at[pl.ds(DV + k, PAIR)]
            send, recv = send_b.at[k // PAIR], recv_b.at[k // PAIR]
        return pltpu.make_async_remote_copy(src_ref=src, dst_ref=dst, send_sem=send, recv_sem=recv,
                                            device_id=place(q), device_id_type=MESH)

    def hops_out(kind, leg):
        up = upward(kind, leg)
        return ((up == 1) & (pos < 3)) | ((up == 0) & (pos > 0))

    def hops_in(kind, leg):
        up = upward(kind, leg)
        return ((up == 1) & (pos > 0)) | ((up == 0) & (pos < 3))

    def f_saves(leg, i):
        pairs = ((a_v, a_hbm), (t_v.at[0], t_hbm), (o_v, o_hbm), (h1_v.at[0], h1_hbm), (n2_v, n2_hbm),
                 (z_v.at[0], z_hbm), (u_v.at[0], u_hbm), (p_v.at[0], p_hbm))
        return [pltpu.make_async_copy(v, h.at[leg, i], fsem.at[n]) for n, (v, h) in enumerate(pairs)]

    def b_saves(leg, i):
        pairs = ((u_v, dz_hbm), (dt_v, dt_hbm), (dh1_v, dh1_hbm), (buf.at[pl.ds(DV + leg * MICRO + i, PAIR)], dh2_hbm))
        return [pltpu.make_async_copy(v, h.at[leg, pl.ds(i, PAIR)], bsem.at[n]) for n, (v, h) in enumerate(pairs)]

    def b_loads(leg, i):
        pairs = ((z_hbm, z_v), (h1_hbm, h1_v), (t_hbm, t_v), (p_hbm, p_v))
        return [pltpu.make_async_copy(h.at[leg, pl.ds(i, PAIR)], v, lsem.at[n]) for n, (h, v) in enumerate(pairs)]

    def to_home(slot, i, dst, send, recv, starting):
        src = buf.at[slot]

        @pl.when(i == 0)
        def _():
            if starting:
                pltpu.make_async_copy(src, dst, recv).start()

        @pl.when((i > 0) & (i < OWN))
        def _():
            rc = pltpu.make_async_remote_copy(src_ref=src, dst_ref=dst, send_sem=send.at[i], recv_sem=recv,
                                              device_id=place(i), device_id_type=MESH)
            if starting:
                rc.start()
            else:
                rc.wait_send()

    lane = lax.broadcasted_iota(jnp.int32, (1, SEQ), 1)
    low = jnp.where(lane < 64, 1.0, 0.0).astype(BF)
    high = jnp.where(lane < 64, 0.0, 1.0).astype(BF)
    q_idx = lax.broadcasted_iota(jnp.int32, (2 * SEQ, SEQ), 0) % SEQ
    k_idx = lax.broadcasted_iota(jnp.int32, (2 * SEQ, SEQ), 1)
    causal = q_idx >= k_idx

    def split_heads(v):
        return jnp.concatenate([v * low, v * high], axis=0)

    def side_by_side(v):
        return jnp.concatenate([v[:SEQ], v[SEQ:]], axis=1)

    def heads(ref, r, part):
        return [ref[r, :, part * DM + p * SEQ:part * DM + (p + 1) * SEQ] for p in range(8)]

    def probs(s):
        s = jnp.where(causal, s * 0.125, NEG)
        e = jnp.exp(s - jnp.max(s, axis=-1, keepdims=True))
        return e * (1.0 / jnp.sum(e, axis=-1, keepdims=True))

    def weights_for(leg, next_leg, fresh, moving):
        def need(*blocks):
            @pl.when(fresh)
            def _():
                for b in blocks:
                    block_copy(b, leg).wait()

        def release(*blocks):
            @pl.when(moving)
            def _():
                for b in blocks:
                    block_copy(b, next_leg).start()

        return need, release

    def forward_task(leg, i, before_kind, before_leg, before_i, need, release):
        c = copy_of(leg)
        k = leg * MICRO + i

        @pl.when((leg == 0) & (pos == 0))
        def _():
            pltpu.make_async_copy(x_hbm, buf.at[HV + i], recv_x.at[i]).wait()

        @pl.when(hops_in(FWD, leg))
        def _():
            hop(FWD, leg, i).wait_recv()

        saves = f_saves(leg, i)
        need(0, 1, 2)
        xh, _ = normalize(buf[HV + k].astype(F32))
        a_v[...] = (xh * vec_ref[c, 0:1, :] + vec_ref[c, 1:2, :]).astype(BF)
        for j in range(3):
            t_v[0, :, block(j)] = (dot_nt(a_v[...], wbuf[j]) + bq_ref[c, :, block(j)]).astype(BF)
        saves[0].start()
        saves[1].start()
        release(0, 1, 2)
        qs = [split_heads(q) for q in heads(t_v, 0, 0)]
        ss = [dot_nt(q, kk) for q, kk in zip(qs, heads(t_v, 0, 1))]
        ps = [probs(sc) for sc in ss]
        for n, (p, v) in enumerate(zip(ps, heads(t_v, 0, 2))):
            p_v[0, n] = p
            o_v[:, n * SEQ:(n + 1) * SEQ] = dot_nn(side_by_side(p.astype(BF)), split_heads(v)).astype(BF)
        saves[2].start()
        saves[7].start()
        need(3)
        h1 = (buf[HV + k].astype(F32) + dot_nn(o_v[...], wbuf[3]) + vec_ref[c, 2:3, :]).astype(BF)
        h1_v[0] = h1
        xh, _ = normalize(h1_v[0].astype(F32))
        n2_v[...] = (xh * vec_ref[c, 3:4, :] + vec_ref[c, 4:5, :]).astype(BF)
        saves[3].start()
        saves[4].start()
        release(3)
        need(4, 5, 6, 7)

        @pl.when(i == 0)
        def _():
            for j in range(4):
                w1_copy(j, leg).wait()

        @pl.when(before_kind == FWD)
        def _():
            for sv in f_saves(before_leg, before_i)[5:7]:
                sv.wait()

        def hidden(j):
            z = dot_nn(n2_v[...], w1buf[leg, j]) + bf_ref[c, :, block(j)]
            zz = z * z
            th = jnp.tanh(z * (GELU_C + GELU_CA * zz))
            half = 0.5 + 0.5 * th
            u_v[0, :, block(j)] = (z * half).astype(BF)
            z_v[0, :, block(j)] = half + ((half * (1.0 - th)) * z) * (GELU_C + (3.0 * GELU_CA) * zz)

        hidden(0)
        acc = jnp.zeros((SEQ, DM), F32)
        for j in range(4):
            if j < 3:
                hidden(j + 1)
            acc = acc + dot_nn(u_v[0, :, block(j)], wbuf[4 + j])
        h2 = (h1_v[0].astype(F32) + (acc + vec_ref[c, 5:6, :])).astype(BF)
        home = (leg == 1) & (pos == 0) & (i < OWN)
        inside = (leg == 0) & (pos == 3)
        buf[jnp.where(home, YO + i, jnp.where(inside, HV + MICRO + i, OUT + k))] = h2

        @pl.when(hops_out(FWD, leg))
        def _():
            hop(FWD, leg, i).start()

        @pl.when(home)
        def _():
            to_home(YO + i, i, y_hbm, send_y, recv_y.at[0], True)

        saves[5].start()
        saves[6].start()
        release(4, 5, 6, 7)

    def backward_task(leg, i, before_kind, before_leg, before_i, next_kind, next_leg, next_i, need, release):
        c = copy_of(leg)
        k = leg * MICRO + i
        loads, later = b_loads(leg, i), b_loads(next_leg, next_i)

        @pl.when(before_kind == FWD)
        def _():
            for ld in loads:
                ld.start()

        def prefetch(n):
            @pl.when(next_kind == BWD)
            def _():
                later[n].start()

        def both(ref_value):
            return ref_value.reshape(ROWS, ref_value.shape[-1])

        def pieces(v):
            return v.reshape(PAIR, SEQ, v.shape[-1])

        @pl.when((leg == 1) & (pos == 0))
        def _():
            for r in range(PAIR):
                pltpu.make_async_copy(dy_hbm, buf.at[DV + k + r], recv_dy.at[i + r]).wait()

        @pl.when(hops_in(BWD, leg))
        def _():
            hop(BWD, leg, i).wait_recv()

        saves = b_saves(leg, i)
        saves[3].start()
        need(4, 5, 6, 7)
        loads[0].wait()

        def tally(ref, row, cols, v):
            ref[c, row:row + 1, cols] += rounded(jnp.sum(v, axis=0, keepdims=True))

        def norm_back(row, before_norm, d_out):
            xh, rstd = normalize(before_norm.astype(F32))
            d_out = rounded(d_out)
            tally(gvec_ref, row, every, d_out * xh)
            tally(gvec_ref, row + 1, every, d_out)
            gx = d_out * vec_ref[c, row:row + 1, :]
            m1 = jnp.mean(gx, axis=-1, keepdims=True)
            m2 = jnp.mean(gx * xh, axis=-1, keepdims=True)
            return rounded(rstd * (gx - m1 - xh * m2))

        every = slice(0, DM)
        dh2 = both(buf[pl.ds(DV + k, PAIR)])

        def hidden(j):
            dz = rounded(dot_nt(dh2, wbuf[4 + j])) * both(z_v[:, :, block(j)])
            for r in range(PAIR):
                tally(gbf_ref, 0, block(j), dz[r * SEQ:(r + 1) * SEQ])
            u_v[:, :, block(j)] = pieces(dz.astype(BF))

        hidden(0)
        dn2 = jnp.zeros((ROWS, DM), F32)
        for j in range(4):
            if j < 3:
                hidden(j + 1)
            dn2 = dn2 + dot_nt(both(u_v[:, :, block(j)]), w1buf[leg, j])
        saves[0].start()
        release(4, 5, 6, 7)
        prefetch(0)
        need(3)
        loads[1].wait()
        for r in range(PAIR):
            dh2f = buf[DV + k + r].astype(F32)
            tally(gvec_ref, 5, every, dh2f)
            dh1_v[r] = (dh2f + norm_back(3, h1_v[r], dn2[r * SEQ:(r + 1) * SEQ])).astype(BF)
            tally(gvec_ref, 2, every, dh1_v[r].astype(F32))
        do_v[...] = pieces(dot_nt(both(dh1_v[...]), wbuf[3]).astype(BF))
        saves[2].start()
        release(3)
        prefetch(1)
        need(0, 1, 2)
        loads[2].wait()
        loads[3].wait()

        @pl.when(before_kind == BWD)
        def _():
            b_saves(before_leg, before_i)[1].wait()

        @pl.when(hops_out(FWD, leg))
        def _():
            for r in range(PAIR):
                hop(FWD, leg, i + r).wait_send()

        def scores_back(r):
            dos = [split_heads(d) for d in heads(do_v, r, 0)]
            dps = [dot_nt(d, v) for d, v in zip(dos, heads(t_v, r, 2))]
            dss = []
            for n, dpv in enumerate(dps):
                p, dpv = p_v[r, n], rounded(dpv)
                dss.append((p * (dpv - jnp.sum(dpv * p, axis=-1, keepdims=True)) * 0.125).astype(BF))
            return dos, dss

        def heads_back(r, dos, dss):
            for n, (q, kk) in enumerate(zip(heads(t_v, r, 0), heads(t_v, r, 1))):
                lo = n * SEQ
                dt_v[r, :, lo:lo + SEQ] = dot_nn(side_by_side(dss[n]), split_heads(kk)).astype(BF)
                dt_v[r, :, DM + lo:DM + lo + SEQ] = dot_tn(dss[n], split_heads(q)).astype(BF)
                dt_v[r, :, 2 * DM + lo:2 * DM + lo + SEQ] = dot_tn(p_v[r, n].astype(BF), dos[n]).astype(BF)

        def input_back(r):
            da = jnp.zeros((SEQ, DM), F32)
            for j in range(3):
                dtj = dt_v[r, :, block(j)]
                tally(gbq_ref, 0, block(j), dtj.astype(F32))
                da = da + dot_nn(dtj, wbuf[j])
            dh = dh1_v[r].astype(F32) + norm_back(0, buf[HV + k + r], da)
            buf[jnp.where((leg == 1) & (pos == 3), DV + i, OUT + k) + r] = dh.astype(BF)

        ahead = [scores_back(r) for r in range(PAIR)]
        for r in range(PAIR):
            heads_back(r, *ahead[r])
            input_back(r)

        @pl.when(hops_out(BWD, leg))
        def _():
            hop(BWD, leg, i).start()

        @pl.when((leg == 0) & (pos == 0))
        def _():
            for r in range(PAIR):
                to_home(OUT + i + r, i + r, dx_hbm, send_dx, recv_dx.at[0], True)

        saves[1].start()
        prefetch(2)
        prefetch(3)
        release(0, 1, 2)

    def slot(s, carry):
        kind, leg, i = parts(code_at(s))
        before_kind, before_leg, before_i = parts(code_at(jnp.maximum(s - 1, 0)))
        next_kind, next_leg, next_i = parts(code_at(jnp.minimum(s + 1, N_TASKS - 1)))
        next_kind = jnp.where(s == N_TASKS - 1, 2, next_kind)
        before_kind = jnp.where(s == 0, 2, before_kind)
        need, release = weights_for(leg, next_leg, (s == 0) | (before_leg != leg), next_leg != leg)

        @pl.when(before_kind == FWD)
        def _():
            for n, sv in enumerate(f_saves(before_leg, before_i)):
                if n not in (5, 6):
                    sv.wait()

        @pl.when(before_kind == BWD)
        def _():
            for n in (0, 2, 3):
                b_saves(before_leg, before_i)[n].wait()

        @pl.when(kind == FWD)
        def _():
            @pl.when(before_kind == BWD)
            def _():
                b_saves(before_leg, before_i)[1].wait()

            forward_task(leg, i, before_kind, before_leg, before_i, need, release)

        @pl.when(kind == BWD)
        def _():
            @pl.when(before_kind == FWD)
            def _():
                for sv in f_saves(before_leg, before_i)[5:7]:
                    sv.wait()

            backward_task(leg, i, before_kind, before_leg, before_i, next_kind, next_leg, next_i, need, release)

        return carry

    lax.fori_loop(0, N_TASKS, slot, 0)
    _, last_leg, last_i = parts(codes[N_TASKS - 1])
    for sv in b_saves(last_leg, last_i):
        sv.wait()

    def finish(n, carry):
        leg, i = n // PAIRS, (n % PAIRS) * PAIR

        @pl.when(hops_out(BWD, leg))
        def _():
            hop(BWD, leg, i).wait_send()

        return carry

    lax.fori_loop(0, 2 * PAIRS, finish, 0)

    @pl.when(pos == 0)
    def _():
        for i in range(OWN):
            to_home(YO + i, jnp.int32(i), y_hbm, send_y, recv_y.at[0], False)
            to_home(OUT + i, jnp.int32(i), dx_hbm, send_dx, recv_dx.at[0], False)

    for src, send in ((x_hbm, send_x), (dy_hbm, send_dy)):
        for n in range(2):
            @pl.when(me != 7 * n)
            def _():
                pltpu.make_async_remote_copy(src_ref=src, dst_ref=buf.at[HV], send_sem=send.at[n], recv_sem=recv_x.at[0],
                                             device_id=(dp, 7 * n), device_id_type=MESH).wait_send()
    pltpu.make_async_copy(buf.at[YO], y_hbm, recv_y.at[0]).wait()
    pltpu.make_async_copy(buf.at[YO], dx_hbm, recv_dx.at[0]).wait()


def run_chain(x, dy, wq, wo, w1, w2, bq, bf, vec):
    hbm = pl.BlockSpec(memory_space=pltpu.HBM)
    vmem = pl.BlockSpec(memory_space=pltpu.VMEM)
    dma = pltpu.SemaphoreType.DMA

    def saved(n, ty=BF):
        return jax.ShapeDtypeStruct((2, MICRO, SEQ, n), ty)

    def paired(n, ty=BF):
        return pltpu.VMEM((PAIR, SEQ, n), ty)

    single = pltpu.VMEM((SEQ, DM), BF)
    return pl.pallas_call(
        chain_kernel,
        out_shape=(
            jax.ShapeDtypeStruct((SEQ, DM), BF), jax.ShapeDtypeStruct((SEQ, DM), BF),
            saved(DM), saved(3 * DM), saved(DM), saved(DM), saved(DM), saved(FF, F32), saved(FF),
            jax.ShapeDtypeStruct((2, MICRO, 8, 2 * SEQ, SEQ), F32),
            saved(FF), saved(3 * DM), saved(DM), saved(DM),
            jax.ShapeDtypeStruct((2, 1, 3 * DM), F32), jax.ShapeDtypeStruct((2, 1, FF), F32), jax.ShapeDtypeStruct((2, 8, DM), F32),
        ),
        in_specs=[hbm] * 6 + [vmem] * 3,
        out_specs=tuple([hbm] * 14 + [vmem] * 3),
        scratch_shapes=[
            pltpu.VMEM((2, 1, 3 * DM), F32), pltpu.VMEM((2, 1, FF), F32), pltpu.VMEM((2, 8, DM), F32),
            pltpu.VMEM((8, DM, DM), BF),
            pltpu.VMEM((2, 4, DM, DM), BF),
            pltpu.VMEM((N_SLOTS, SEQ, DM), BF),
            single, paired(3 * DM), single, paired(DM), single, paired(FF, F32), paired(FF),
            pltpu.VMEM((PAIR, 8, 2 * SEQ, SEQ), F32), paired(3 * DM), paired(DM), paired(DM),
            dma((8,)), dma((8,)), dma((8,)), dma((4,)), dma((4,)), dma((MICRO,)), dma((MICRO,)), dma((2,)), dma((2,)),
            dma((2 * MICRO,)), dma((2 * MICRO,)), dma((2 * PAIRS,)), dma((2 * PAIRS,)),
            dma((OWN,)), dma((1,)), dma((OWN,)), dma((1,)),
        ],
        compiler_params=pltpu.CompilerParams(collective_id=0, has_side_effects=True, vmem_limit_bytes=67000000),
        name="chain",
    )(x, dy, wq, wo, w1, w2, bq, bf, vec)


N_TILES = 24
STRIP = 256


def wgrad_kernel(dt_hbm, a_hbm, o_hbm, dh1_hbm, n2_hbm, dz_hbm, u_hbm, dh2_hbm, y_in, dx_in, gbq_in, gbf_in, gvec_in,
                 gq_hbm, go_hbm, g1_hbm, g2_hbm, y_hbm, dx_hbm, gbq_ref, gbf_ref, gvec_ref, l_v, r_v, out_v, pass_v,
                 lsem, rsem, osem, psem):
    side = lax.axis_index('pp') // 4

    def tile(n, act):
        leg, b = n // 12, n % 12
        c = leg + side - 2 * leg * side
        at = n % 2

        def cols(j):
            return pl.ds(pl.multiple_of(j * DM, DM), DM)

        def three(left, right, out):
            if act == 'load':
                pltpu.make_async_copy(left, l_v.at[at], lsem.at[at]).start()
                pltpu.make_async_copy(right, r_v.at[at], rsem.at[at]).start()
            else:
                pltpu.make_async_copy(out_v.at[at], out, osem.at[at]).start()

        @pl.when(b < 3)
        def _():
            three(dt_hbm.at[leg, :, :, cols(b)], a_hbm.at[leg], gq_hbm.at[c, cols(b), :])

        @pl.when(b == 3)
        def _():
            three(o_hbm.at[leg], dh1_hbm.at[leg], go_hbm.at[c])

        @pl.when((b > 3) & (b < 8))
        def _():
            j = b - 4
            three(n2_hbm.at[leg], dz_hbm.at[leg, :, :, cols(j)], g1_hbm.at[c, :, cols(j)])

        @pl.when(b > 7)
        def _():
            j = b - 8
            three(u_hbm.at[leg, :, :, cols(j)], dh2_hbm.at[leg], g2_hbm.at[c, cols(j), :])

    tile(jnp.int32(0), 'load')

    def passing(act):
        for n, (src, dst) in enumerate(((y_in, y_hbm), (dx_in, dx_hbm))):
            into = pltpu.make_async_copy(src, pass_v.at[n], psem.at[n])
            out = pltpu.make_async_copy(pass_v.at[n], dst, psem.at[n])
            if act == 'in':
                into.start()
            elif act == 'out':
                into.wait()
                out.start()
            else:
                out.wait()

    passing('in')
    gbf_ref[...] = gbf_in[...]
    for c in range(2):
        for n in range(6):
            gvec_ref[c, n] = gvec_in[c, n:n + 1, :]
        for n in range(48):
            gbq_ref[c, n // 16, n % 16:n % 16 + 1, :] = gbq_in[c, :, n * 64:(n + 1) * 64]
    passing('out')

    def step(n, carry):
        at = n % 2

        @pl.when(n + 1 < N_TILES)
        def _():
            tile(n + 1, 'load')

        pltpu.make_async_copy(a_hbm.at[0], l_v.at[at], lsem.at[at]).wait()
        pltpu.make_async_copy(a_hbm.at[0], r_v.at[at], rsem.at[at]).wait()

        @pl.when(n > 1)
        def _():
            pltpu.make_async_copy(out_v.at[at], go_hbm.at[0], osem.at[at]).wait()

        for k in range(DM // STRIP):
            rows = slice(k * STRIP, (k + 1) * STRIP)
            acc = rounded(dot_nn(l_v[at, 0, :, rows].T, r_v[at, 0]))
            for m in range(1, MICRO):
                acc = acc + rounded(dot_nn(l_v[at, m, :, rows].T, r_v[at, m]))
            out_v[at, rows, :] = acc
        tile(n, 'store')
        return carry

    lax.fori_loop(0, N_TILES, step, 0)
    for at in range(2):
        pltpu.make_async_copy(out_v.at[at], go_hbm.at[0], osem.at[at]).wait()
    passing('done')


def weight_grads(*saved):
    hbm = pl.BlockSpec(memory_space=pltpu.HBM)
    vmem = pl.BlockSpec(memory_space=pltpu.VMEM)
    dma = pltpu.SemaphoreType.DMA
    return pl.pallas_call(
        wgrad_kernel,
        out_shape=tuple(jax.ShapeDtypeStruct((2,) + s, F32) for s in ((3 * DM, DM), (DM, DM), (DM, FF), (FF, DM)))
        + (jax.ShapeDtypeStruct((SEQ, DM), BF),) * 2
        + tuple(jax.ShapeDtypeStruct((2,) + s, F32) for s in ((3, 16, 64), (1, FF), (6, 1, DM))),
        in_specs=[hbm] * 10 + [vmem] * 3,
        out_specs=tuple([hbm] * 6 + [vmem] * 3),
        scratch_shapes=[
            pltpu.VMEM((2, MICRO, SEQ, DM), BF), pltpu.VMEM((2, MICRO, SEQ, DM), BF), pltpu.VMEM((2, DM, DM), F32),
            pltpu.VMEM((2, SEQ, DM), BF), dma((2,)), dma((2,)), dma((2,)), dma((2,)),
        ],
        compiler_params=pltpu.CompilerParams(vmem_limit_bytes=67000000),
        cost_estimate=pl.CostEstimate(flops=4 * MICRO * SEQ * 12 * DM * DM, bytes_accessed=N_TILES * 8 * DM * DM, transcendentals=0),
        name="wgrad",
    )(*saved)


def solution(mesh):
    data_spec = P(('dp', 'pp'))
    weight_spec = P('pp')

    def per_device(x_loc, dy_loc, w_qkv, w_attn, w_fc, w_proj, b_qkv, b_fc, vec_d):
        wq = jnp.transpose(w_qkv, (0, 1, 2, 4, 5, 6, 3)).reshape(2, 3 * DM, DM)
        bq = b_qkv.reshape(2, 3, 16, 64)
        bf = b_fc.reshape(2, FF)
        vec = jnp.transpose(vec_d.reshape(2, 6, DM), (1, 0, 2))
        (y, dx, a, _, o, _, n2, _, u, _, dz, dt, dh1, dh2, gbq, gbf, gvec) = run_chain(
            x_loc.reshape(SEQ, DM), dy_loc.reshape(SEQ, DM), wq, w_attn.reshape(2, DM, DM), w_fc.reshape(2, DM, FF),
            w_proj.reshape(2, FF, DM), bq, bf, vec)
        gq, go, g1, g2, y, dx, gbq, gbf, gvec = weight_grads(dt, a, o, dh1, n2, dz, u, dh2, y, dx, gbq, gbf, gvec)
        gq = jnp.transpose(gq.reshape(1, 2, 1, 3, 16, 64, DM), (0, 1, 2, 6, 3, 4, 5))
        return (
            y.reshape(x_loc.shape), dx.reshape(x_loc.shape), gq, go.reshape(w_attn.shape), g1.reshape(w_fc.shape),
            g2.reshape(w_proj.shape), gbq.reshape(b_qkv.shape), gbf.reshape(b_fc.shape), gvec.reshape(vec_d.shape),
        )

    return jax.shard_map(per_device, mesh=mesh, in_specs=(data_spec, data_spec) + (weight_spec,) * 7,
                         out_specs=(data_spec, data_spec) + (data_spec,) * 7, check_vma=False)
```

```python
import jax
import jax.numpy as jnp
from jax import lax
from jax.experimental import pallas as pl
from jax.experimental.pallas import tpu as pltpu
from jax.sharding import PartitionSpec as P

EPSILON = 1e-5
SEQ = 128
DM = 1024
FF = 4096
MICRO = 8
OWN = MICRO // 2
PAIR = 2
HV, DV, OUT, YO = 0, 2 * MICRO, 4 * MICRO, 4 * MICRO + 2 * OWN
D1 = YO + OWN
N_SLOTS = D1 + 2 * OWN
FWD, BWD, FWD_FAR, BWD_FAR, NONE = 0, 1, 2, 3, 4
N_TASKS = 24
ORDER = (
    (0x2da2ac6496080c1080, 0xdb44d2411fa693cb9b),
    (0x2d9298248983901080, 0xfb6d1349047cbac6da),
    (0xb982e42ac243201080, 0xfb4da64d24116daf19),
    (0x418bac2c3282241200, 0xfbcd369a44db49a459),
)
GELU_C = 0.7978845608028654
GELU_CA = GELU_C * 0.044715
NEG = -1e30
MESH = pl.DeviceIdType.MESH
BF = jnp.bfloat16
F32 = jnp.float32


def dot_nn(a, b):
    return lax.dot_general(a, b, (((1,), (0,)), ((), ())), preferred_element_type=F32)


def dot_nt(a, b):
    return lax.dot_general(a, b, (((1,), (1,)), ((), ())), preferred_element_type=F32)


def dot_tn(a, b):
    return lax.dot_general(a, b, (((0,), (0,)), ((), ())), preferred_element_type=F32)


def normalize(rows_f32):
    mean = jnp.mean(rows_f32, axis=-1, keepdims=True)
    centered = rows_f32 - mean
    var = jnp.mean(centered * centered, axis=-1, keepdims=True)
    rstd = lax.rsqrt(var + EPSILON)
    return centered * rstd, rstd


def rounded(v):
    return v.astype(BF).astype(F32)


def gelu_parts(z):
    zz = z * z
    th = jnp.tanh(z * (GELU_C + GELU_CA * zz))
    half = 0.5 + 0.5 * th
    return half, half + ((half * (1.0 - th)) * z) * (GELU_C + (3.0 * GELU_CA) * zz)


def block(j):
    return slice(j * DM, (j + 1) * DM)


def chain_kernel(x_hbm, dy_hbm, wq_hbm, wo_hbm, w1_hbm, w2_hbm, bq_in, bf_in, vec_in,
                 y_hbm, dx_hbm, a_hbm, t_hbm, o_hbm, h1_hbm, n2_hbm, z_hbm, u_hbm, p_hbm,
                 dz_hbm, dt_hbm, dh1_hbm, dh2_hbm, gbq_ref, gbf_ref, gvec_ref,
                 bq_ref, bf_ref, vec_ref, wbuf, w1buf, buf, a_v, t_v, o_v, h1_v, n2_v, z_v, u_v, p_v, dt_v, dh1_v, do_v, gln_v, gln_far,
                 wsem, w1sem, fsem, bsem, lsem, recv_x, recv_dy, send_x, send_dy,
                 send_f, recv_f, send_b, recv_b, send_fm, recv_fm, send_bm, recv_bm, send_d1, recv_d1, send_g, recv_g, send_y, recv_y, send_dx, recv_dx):
    me = lax.axis_index('pp')
    dp = lax.axis_index('dp')
    side = me // 4
    pos = me + side * (7 - 2 * me)

    def place(q):
        return (dp, q + side * (7 - 2 * q))

    def copy_of(leg):
        return leg + side - 2 * leg * side

    codes = []
    for s in range(N_TASKS):
        row = [jnp.int32((ORDER[q][s // 12] >> (6 * (s % 12))) % 64) for q in range(4)]
        codes.append(jnp.where(pos == 0, row[0], jnp.where(pos == 1, row[1], jnp.where(pos == 2, row[2], row[3]))))

    def code_at(s):
        c = codes[0]
        for k in range(1, N_TASKS):
            c = jnp.where(s == k, codes[k], c)
        return c

    def parts(code):
        return code // 16, (code // 8) % 2, code % 8

    barrier = pltpu.get_barrier_semaphore()
    for k in range(1, 8):
        pl.semaphore_signal(barrier, inc=1, device_id=(dp, lax.rem(me + k, 8)), device_id_type=MESH)

    def block_copy(b, leg):
        c = copy_of(leg)
        if b < 3:
            src = wq_hbm.at[c, pl.ds(b * DM, DM), :]
        elif b == 3:
            src = wo_hbm.at[c]
        else:
            src = w2_hbm.at[c, pl.ds((b - 4) * DM, DM), :]
        return pltpu.make_async_copy(src, wbuf.at[b], wsem.at[b])

    def w1_copy(j, leg):
        return pltpu.make_async_copy(w1_hbm.at[copy_of(leg), :, pl.ds(j * DM, DM)], w1buf.at[leg, j], w1sem.at[leg * 4 + j])

    first_leg = parts(codes[0])[1]
    for b in range(4):
        block_copy(b, first_leg).start()
    for j in range(4):
        w1_copy(j, first_leg).start()
        block_copy(4 + j, first_leg).start()
    for j in range(4):
        w1_copy(j, 1 - first_leg).start()

    for c in range(2):
        bf_ref[c] = bf_in[c:c + 1, :].astype(F32)
        for n in range(6):
            vec_ref[c, n:n + 1, :] = vec_in[n, c:c + 1, :].astype(F32)
        for n in range(24):
            pair = bq_in[c, n // 8, 2 * (n % 8):2 * (n % 8) + 2, :].astype(F32)
            bq_ref[c, :, n * SEQ:(n + 1) * SEQ] = jnp.concatenate([pair[:1], pair[1:]], axis=1)
    gbq_ref[...] = jnp.zeros_like(gbq_ref)
    gbf_ref[...] = jnp.zeros_like(gbf_ref)
    gln_v[...] = jnp.zeros_like(gln_v)

    pl.semaphore_wait(barrier, 7)

    def spread(src, base, send, recv):
        dst = buf.at[base + pos]

        @pl.when(pos == 0)
        def _():
            pltpu.make_async_copy(src, dst, recv.at[0]).start()

        @pl.when(pos != 0)
        def _():
            pltpu.make_async_remote_copy(src_ref=src, dst_ref=dst, send_sem=send.at[0], recv_sem=recv.at[pos],
                                         device_id=place(0), device_id_type=MESH).start()

    spread(x_hbm, HV, send_x, recv_x)
    spread(dy_hbm, DV + MICRO, send_dy, recv_dy)

    def upward(kind, leg):
        return leg if kind == BWD else 1 - leg

    def hop(kind, leg, i):
        k, n = leg * MICRO + i, leg * OWN + i
        q = pos - 1 + 2 * upward(kind, leg)
        base, send, recv = (HV, send_f, recv_f) if kind == FWD else (DV, send_b, recv_b)
        return pltpu.make_async_remote_copy(src_ref=buf.at[OUT + n], dst_ref=buf.at[base + k], send_sem=send.at[n],
                                            recv_sem=recv.at[n], device_id=place(q), device_id_type=MESH)

    def mirror(kind, leg, i):
        k, n = leg * MICRO + i, leg * OWN + i
        base, send, recv = (HV, send_fm, recv_fm) if kind == FWD else (DV, send_bm, recv_bm)
        return pltpu.make_async_remote_copy(src_ref=buf.at[base + k], dst_ref=buf.at[base + k + OWN], send_sem=send.at[n],
                                            recv_sem=recv.at[n], device_id=(dp, 7 - me), device_id_type=MESH)

    def mirror_dh1(leg, i):
        n = leg * OWN + i
        return pltpu.make_async_remote_copy(src_ref=dh1_v.at[0], dst_ref=buf.at[D1 + n], send_sem=send_d1.at[0],
                                            recv_sem=recv_d1.at[n], device_id=(dp, 7 - me), device_id_type=MESH)

    def mirror_sums():
        return pltpu.make_async_remote_copy(src_ref=gln_v, dst_ref=gln_far, send_sem=send_g.at[0], recv_sem=recv_g.at[0],
                                            device_id=(dp, 7 - me), device_id_type=MESH)

    def hops_out(kind, leg):
        up = upward(kind, leg)
        return ((up == 1) & (pos < 3)) | ((up == 0) & (pos > 0))

    def hops_in(kind, leg):
        up = upward(kind, leg)
        return ((up == 1) & (pos > 0)) | ((up == 0) & (pos < 3))

    def f_saves(leg, i, n):
        pairs = ((a_v, a_hbm), (t_v, t_hbm), (o_v, o_hbm), (h1_v, h1_hbm), (n2_v, n2_hbm), (z_v, z_hbm), (u_v, u_hbm), (p_v, p_hbm))
        return [pltpu.make_async_copy(v.at[pl.ds(0, n)], h.at[leg, pl.ds(i, n)], fsem.at[m]) for m, (v, h) in enumerate(pairs)]

    def flush_forward(kind, leg, i, which):
        for n, of_kind in ((1, FWD), (PAIR, FWD_FAR)):
            @pl.when(kind == of_kind)
            def _():
                saves = f_saves(leg, i, n)
                for m in which:
                    if n == 1 or m != 3:
                        saves[m].wait()

    def b_saves(leg, i, n):
        own = pl.ds(0, n)
        dh1 = dh1_v if n == 1 else buf.at[pl.ds(D1 + leg * OWN + i - OWN, n)]
        pairs = ((u_v.at[pl.ds(PAIR - n, n)], dz_hbm), (dt_v.at[own], dt_hbm), (dh1, dh1_hbm), (buf.at[pl.ds(DV + leg * MICRO + i, n)], dh2_hbm))
        return [pltpu.make_async_copy(v, h.at[leg, pl.ds(i, n)], bsem.at[m]) for m, (v, h) in enumerate(pairs)]

    def b_loads(leg, i, n):
        pairs = ((z_hbm, z_v), (h1_hbm, h1_v), (t_hbm, t_v), (p_hbm, p_v))
        return [pltpu.make_async_copy(h.at[leg, pl.ds(i, n)], v.at[pl.ds(0, n)], lsem.at[m]) for m, (h, v) in enumerate(pairs)]

    def flush_backward(kind, leg, i, which):
        for n, of_kind in ((1, BWD), (PAIR, BWD_FAR)):
            @pl.when(kind == of_kind)
            def _():
                saves = b_saves(leg, i, n)
                for m in which:
                    saves[m].wait()

    def to_home(slot, i, dst, send, recv, starting):
        src = buf.at[slot]

        @pl.when(i == 0)
        def _():
            if starting:
                pltpu.make_async_copy(src, dst, recv).start()

        @pl.when((i > 0) & (i < OWN))
        def _():
            rc = pltpu.make_async_remote_copy(src_ref=src, dst_ref=dst, send_sem=send.at[i], recv_sem=recv,
                                              device_id=place(i), device_id_type=MESH)
            if starting:
                rc.start()
            else:
                rc.wait_send()

    lane = lax.broadcasted_iota(jnp.int32, (1, SEQ), 1)
    low = jnp.where(lane < 64, 1.0, 0.0).astype(BF)
    high = jnp.where(lane < 64, 0.0, 1.0).astype(BF)
    q_idx = lax.broadcasted_iota(jnp.int32, (2 * SEQ, SEQ), 0) % SEQ
    k_idx = lax.broadcasted_iota(jnp.int32, (2 * SEQ, SEQ), 1)
    causal = q_idx >= k_idx

    def split_heads(v):
        return jnp.concatenate([v * low, v * high], axis=0)

    def side_by_side(v):
        return jnp.concatenate([v[:SEQ], v[SEQ:]], axis=1)

    def heads(ref, r, part):
        return [ref[r, :, part * DM + p * SEQ:part * DM + (p + 1) * SEQ] for p in range(8)]

    def probs(s):
        s = jnp.where(causal, s * 0.125, NEG)
        e = jnp.exp(s - jnp.max(s, axis=-1, keepdims=True))
        return e * (1.0 / jnp.sum(e, axis=-1, keepdims=True))

    def weights_for(leg, next_leg, fresh, moving):
        def need(*blocks):
            @pl.when(fresh)
            def _():
                for b in blocks:
                    block_copy(b, leg).wait()

        def release(*blocks):
            @pl.when(moving)
            def _():
                for b in blocks:
                    block_copy(b, next_leg).start()

        return need, release

    def flat(v):
        return v.reshape(v.shape[0] * v.shape[1], v.shape[2])

    def pieces(v):
        return v.reshape(v.shape[0] // SEQ, SEQ, v.shape[1])

    def forward_task(n, far, leg, i, before_kind, before_leg, before_i, need, release):
        c = copy_of(leg)
        k = leg * MICRO + i
        own = slice(0, n)

        if far:
            for r in range(n):
                mirror(FWD, leg, i - OWN + r).wait_recv()
        else:
            @pl.when((leg == 0) & (pos == 0))
            def _():
                pltpu.make_async_copy(x_hbm, buf.at[HV + i], recv_x.at[i]).wait()

            @pl.when(hops_in(FWD, leg))
            def _():
                hop(FWD, leg, i).wait_recv()

            mirror(FWD, leg, i).start()

        saves = f_saves(leg, i, n)
        need(0, 1, 2)
        xh, _ = normalize(flat(buf[pl.ds(HV + k, n)]).astype(F32))
        a_v[own] = pieces((xh * vec_ref[c, 0:1, :] + vec_ref[c, 1:2, :]).astype(BF))
        for j in range(3):
            t_v[own, :, block(j)] = pieces((dot_nt(flat(a_v[own]), wbuf[j]) + bq_ref[c, :, block(j)]).astype(BF))
        saves[0].start()
        saves[1].start()
        release(0, 1, 2)
        ss = [[dot_nt(split_heads(q), kk) for q, kk in zip(heads(t_v, r, 0), heads(t_v, r, 1))] for r in range(n)]
        ps = [[probs(sc) for sc in row] for row in ss]
        for r in range(n):
            for m, (p, v) in enumerate(zip(ps[r], heads(t_v, r, 2))):
                p_v[r, m] = p
                o_v[r, :, m * SEQ:(m + 1) * SEQ] = dot_nn(side_by_side(p.astype(BF)), split_heads(v)).astype(BF)
        saves[2].start()
        saves[7].start()
        need(3)
        h1 = flat(buf[pl.ds(HV + k, n)]).astype(F32) + dot_nn(flat(o_v[own]), wbuf[3]) + vec_ref[c, 2:3, :]
        h1_v[own] = pieces(h1.astype(BF))
        xh, _ = normalize(flat(h1_v[own]).astype(F32))
        n2_v[own] = pieces((xh * vec_ref[c, 3:4, :] + vec_ref[c, 4:5, :]).astype(BF))
        if not far:
            saves[3].start()
        saves[4].start()
        release(3)
        need(4, 5, 6, 7)

        @pl.when(i == 0)
        def _():
            for j in range(4):
                w1_copy(j, leg).wait()

        flush_forward(before_kind, before_leg, before_i, (5, 6))

        def hidden(j):
            z = dot_nn(flat(n2_v[own]), w1buf[leg, j]) + bf_ref[c, :, block(j)]
            half, slope = gelu_parts(z)
            u_v[own, :, block(j)] = pieces((z * half).astype(BF))
            z_v[own, :, block(j)] = pieces(z if far else slope)

        hidden(0)
        acc = jnp.zeros((n * SEQ, DM), F32)
        for j in range(4):
            if j < 3:
                hidden(j + 1)
            if not far:
                acc = acc + dot_nn(flat(u_v[own, :, block(j)]), wbuf[4 + j])
        if not far:
            h2 = (flat(h1_v[own]).astype(F32) + (acc + vec_ref[c, 5:6, :])).astype(BF)
            home = (leg == 1) & (pos == 0)
            inside = (leg == 0) & (pos == 3)
            buf[jnp.where(home, YO + i, jnp.where(inside, HV + MICRO + i, OUT + leg * OWN + i))] = h2

            @pl.when(hops_out(FWD, leg))
            def _():
                hop(FWD, leg, i).start()

            @pl.when(home)
            def _():
                to_home(YO + i, i, y_hbm, send_y, recv_y.at[0], True)

        saves[5].start()
        saves[6].start()
        release(4, 5, 6, 7)

    def backward_task(n, far, leg, i, before_kind, before_leg, before_i, next_kind, next_leg, next_i, need, release):
        c = copy_of(leg)
        k = leg * MICRO + i
        own, dz_at = slice(0, n), slice(PAIR - n, PAIR)
        loads = b_loads(leg, i, n)

        after_b = (before_kind == BWD) | (before_kind == BWD_FAR)

        inplace = (before_kind == FWD) & (before_leg == leg) & (before_i == i) & (not far)

        @pl.when(jnp.logical_not(inplace))
        def _():
            flush_forward(before_kind, before_leg, before_i, (5, 6))

        @pl.when(jnp.logical_not(after_b | inplace))
        def _():
            for m, ld in enumerate(loads):
                if m != 1 or not far:
                    ld.start()

        def arrived(*which):
            @pl.when(jnp.logical_not(inplace))
            def _():
                for m in which:
                    loads[m].wait()

        def prefetch(m):
            for next_n, of_kind in ((1, BWD), (PAIR, BWD_FAR)):
                if m != 1 or of_kind == BWD:
                    @pl.when(next_kind == of_kind)
                    def _():
                        b_loads(next_leg, next_i, next_n)[m].start()

        if far:
            for r in range(n):
                mirror(BWD, leg, i - OWN + r).wait_recv()
        else:
            @pl.when((leg == 1) & (pos == 0))
            def _():
                pltpu.make_async_copy(dy_hbm, buf.at[DV + k], recv_dy.at[i]).wait()

            @pl.when(hops_in(BWD, leg))
            def _():
                hop(BWD, leg, i).wait_recv()

            mirror(BWD, leg, i).start()

        def tally(ref, at, row, cols, v):
            ref[at, row:row + 1, cols] += rounded(jnp.sum(v, axis=0, keepdims=True))

        saves = b_saves(leg, i, n)
        saves[3].start()
        need(4, 5, 6, 7)
        if far:
            arrived(0)
        else:
            arrived(0, 1)
            second_norm = normalize(h1_v[0].astype(F32))
            first_norm = normalize(buf[HV + k].astype(F32))
            tally(gln_v, leg, 5, slice(0, DM), buf[DV + k].astype(F32))

        def norm_back(row, normalized, d_out):
            xh, rstd = normalized
            d_out = rounded(d_out)
            tally(gln_v, leg, row, every, d_out * xh)
            tally(gln_v, leg, row + 1, every, d_out)
            gx = d_out * vec_ref[c, row:row + 1, :]
            m1 = jnp.mean(gx, axis=-1, keepdims=True)
            m2 = jnp.mean(gx * xh, axis=-1, keepdims=True)
            return rounded(rstd * (gx - m1 - xh * m2))

        every = slice(0, DM)
        dh2 = flat(buf[pl.ds(DV + k, n)])

        def hidden(j):
            z = flat(z_v[own, :, block(j)])
            dz = rounded(dot_nt(dh2, wbuf[4 + j])) * (gelu_parts(z)[1] if far else z)
            for r in range(n):
                tally(gbf_ref, c, 0, block(j), dz[r * SEQ:(r + 1) * SEQ])
            u_v[dz_at, :, block(j)] = pieces(dz.astype(BF))

        hidden(0)
        dn2 = jnp.zeros((n * SEQ, DM), F32)
        for j in range(4):
            if j < 3:
                hidden(j + 1)
            if not far:
                dn2 = dn2 + dot_nt(flat(u_v[dz_at, :, block(j)]), w1buf[leg, j])
        saves[0].start()
        release(4, 5, 6, 7)
        prefetch(0)
        need(3)
        if far:
            for r in range(n):
                mirror_dh1(leg, i - OWN + r).wait_recv()
            dh1 = flat(buf[pl.ds(D1 + leg * OWN + i - OWN, n)])
        else:
            @pl.when((leg == 0) | (i > 0))
            def _():
                mirror_dh1(leg, i).wait_send()

            dh1_v[0] = (buf[DV + k].astype(F32) + norm_back(3, second_norm, dn2)).astype(BF)
            mirror_dh1(leg, i).start()
            dh1 = dh1_v[0]
            tally(gln_v, leg, 2, every, dh1.astype(F32))
        do_v[own] = pieces(dot_nt(dh1, wbuf[3]).astype(BF))
        saves[2].start()
        release(3)
        prefetch(1)
        need(0, 1, 2)
        arrived(2, 3)

        @pl.when(inplace)
        def _():
            flush_forward(before_kind, before_leg, before_i, (5, 6))

        flush_backward(before_kind, before_leg, before_i, (1,))
        if not far:
            @pl.when(hops_out(FWD, leg))
            def _():
                hop(FWD, leg, i).wait_send()

        def scores_back(r):
            dos = [split_heads(d) for d in heads(do_v, r, 0)]
            dps = [dot_nt(d, v) for d, v in zip(dos, heads(t_v, r, 2))]
            dss = []
            for m, dpv in enumerate(dps):
                p, dpv = p_v[r, m], rounded(dpv)
                dss.append((p * (dpv - jnp.sum(dpv * p, axis=-1, keepdims=True)) * 0.125).astype(BF))
            return dos, dss

        def heads_back(r, dos, dss):
            for m, (q, kk) in enumerate(zip(heads(t_v, r, 0), heads(t_v, r, 1))):
                lo = m * SEQ
                dt_v[r, :, lo:lo + SEQ] = dot_nn(side_by_side(dss[m]), split_heads(kk)).astype(BF)
                dt_v[r, :, DM + lo:DM + lo + SEQ] = dot_tn(dss[m], split_heads(q)).astype(BF)
                dt_v[r, :, 2 * DM + lo:2 * DM + lo + SEQ] = dot_tn(p_v[r, m].astype(BF), dos[m]).astype(BF)

        def input_back(r):
            da = jnp.zeros((SEQ, DM), F32)
            for j in range(3):
                dtj = dt_v[r, :, block(j)]
                tally(gbq_ref, c, 0, block(j), dtj.astype(F32))
                if not far:
                    da = da + dot_nn(dtj, wbuf[j])
            if not far:
                dh = dh1_v[r].astype(F32) + norm_back(0, first_norm, da)
                buf[jnp.where((leg == 1) & (pos == 3), DV + i, OUT + leg * OWN + i) + r] = dh.astype(BF)

        ahead = [scores_back(r) for r in range(n)]
        for r in range(n):
            heads_back(r, *ahead[r])
            input_back(r)

        if not far:
            @pl.when(hops_out(BWD, leg))
            def _():
                hop(BWD, leg, i).start()

            @pl.when((leg == 0) & (pos == 0))
            def _():
                to_home(OUT + i, i, dx_hbm, send_dx, recv_dx.at[0], True)

            @pl.when((leg == 0) & (i == OWN - 1))
            def _():
                mirror_sums().start()

        saves[1].start()
        prefetch(2)
        prefetch(3)
        release(0, 1, 2)

    def slot(s, carry):
        kind, leg, i = parts(code_at(s))
        before_kind, before_leg, before_i = parts(code_at(jnp.maximum(s - 1, 0)))
        next_kind, next_leg, next_i = parts(code_at(jnp.minimum(s + 1, N_TASKS - 1)))
        next_kind = jnp.where(s == N_TASKS - 1, NONE, next_kind)
        before_kind = jnp.where(s == 0, NONE, before_kind)
        need, release = weights_for(leg, next_leg, (s == 0) | (before_leg != leg), next_leg != leg)
        flush_forward(before_kind, before_leg, before_i, (0, 1, 2, 3, 4, 7))

        flush_backward(before_kind, before_leg, before_i, (0, 2, 3))
        for n, of_kind in ((1, FWD), (PAIR, FWD_FAR)):
            @pl.when(kind == of_kind)
            def _():
                flush_backward(before_kind, before_leg, before_i, (1,))
                forward_task(n, of_kind == FWD_FAR, leg, i, before_kind, before_leg, before_i, need, release)

        for n, of_kind in ((1, BWD), (PAIR, BWD_FAR)):
            @pl.when(kind == of_kind)
            def _():
                backward_task(n, of_kind == BWD_FAR, leg, i, before_kind, before_leg, before_i, next_kind, next_leg, next_i, need, release)

        return carry

    lax.fori_loop(0, N_TASKS, slot, 0)
    flush_backward(*parts(codes[N_TASKS - 1]), (0, 1, 2, 3))
    for leg in range(2):
        for i in range(OWN):
            mirror(FWD, leg, i).wait_send()
            mirror(BWD, leg, i).wait_send()

            @pl.when(hops_out(BWD, leg))
            def _():
                hop(BWD, leg, i).wait_send()

    @pl.when(pos == 0)
    def _():
        for i in range(OWN):
            to_home(YO + i, jnp.int32(i), y_hbm, send_y, recv_y.at[0], False)
            to_home(OUT + i, jnp.int32(i), dx_hbm, send_dx, recv_dx.at[0], False)

    @pl.when(pos != 0)
    def _():
        for src, send in ((x_hbm, send_x), (dy_hbm, send_dy)):
            pltpu.make_async_remote_copy(src_ref=src, dst_ref=buf.at[HV], send_sem=send.at[0], recv_sem=recv_x.at[0],
                                         device_id=place(0), device_id_type=MESH).wait_send()

    mirror_dh1(0, OWN - 1).wait_send()
    mirror_sums().wait()
    for leg in range(2):
        gvec_ref[copy_of(leg)] = gln_v[leg] + gln_far[leg]
    pltpu.make_async_copy(buf.at[YO], y_hbm, recv_y.at[0]).wait()
    pltpu.make_async_copy(buf.at[YO], dx_hbm, recv_dx.at[0]).wait()


def run_chain(x, dy, wq, wo, w1, w2, bq, bf, vec):
    hbm = pl.BlockSpec(memory_space=pltpu.HBM)
    vmem = pl.BlockSpec(memory_space=pltpu.VMEM)
    dma = pltpu.SemaphoreType.DMA

    def saved(n, ty=BF):
        return jax.ShapeDtypeStruct((2, MICRO, SEQ, n), ty)

    def paired(n, ty=BF):
        return pltpu.VMEM((PAIR, SEQ, n), ty)

    return pl.pallas_call(
        chain_kernel,
        out_shape=(
            jax.ShapeDtypeStruct((SEQ, DM), BF), jax.ShapeDtypeStruct((SEQ, DM), BF),
            saved(DM), saved(3 * DM), saved(DM), saved(DM), saved(DM), saved(FF, F32), saved(FF),
            jax.ShapeDtypeStruct((2, MICRO, 8, 2 * SEQ, SEQ), F32),
            saved(FF), saved(3 * DM), saved(DM), saved(DM),
            jax.ShapeDtypeStruct((2, 1, 3 * DM), F32), jax.ShapeDtypeStruct((2, 1, FF), F32), jax.ShapeDtypeStruct((2, 8, DM), F32),
        ),
        in_specs=[hbm] * 6 + [vmem] * 3,
        out_specs=tuple([hbm] * 14 + [vmem] * 3),
        scratch_shapes=[
            pltpu.VMEM((2, 1, 3 * DM), F32), pltpu.VMEM((2, 1, FF), F32), pltpu.VMEM((2, 8, DM), F32),
            pltpu.VMEM((8, DM, DM), BF),
            pltpu.VMEM((2, 4, DM, DM), BF),
            pltpu.VMEM((N_SLOTS, SEQ, DM), BF),
            paired(DM), paired(3 * DM), paired(DM), paired(DM), paired(DM), paired(FF, F32), paired(FF),
            pltpu.VMEM((PAIR, 8, 2 * SEQ, SEQ), F32), paired(3 * DM), pltpu.VMEM((1, SEQ, DM), BF), paired(DM),
            pltpu.VMEM((2, 8, DM), F32), pltpu.VMEM((2, 8, DM), F32),
            dma((8,)), dma((8,)), dma((8,)), dma((4,)), dma((4,)), dma((OWN,)), dma((OWN,)), dma((1,)), dma((1,)),
            *[dma((2 * OWN,))] * 8, dma((1,)), dma((2 * OWN,)), dma((1,)), dma((1,)),
            dma((OWN,)), dma((1,)), dma((OWN,)), dma((1,)),
        ],
        compiler_params=pltpu.CompilerParams(collective_id=0, has_side_effects=True, vmem_limit_bytes=67000000),
        name="chain",
    )(x, dy, wq, wo, w1, w2, bq, bf, vec)


N_TILES = 24
STRIP = 256


def wgrad_kernel(dt_hbm, a_hbm, o_hbm, dh1_hbm, n2_hbm, dz_hbm, u_hbm, dh2_hbm, y_in, dx_in, gbq_in, gbf_in, gvec_in,
                 gq_hbm, go_hbm, g1_hbm, g2_hbm, y_hbm, dx_hbm, gbq_ref, gbf_ref, gvec_ref, l_v, r_v, out_v, pass_v,
                 lsem, rsem, osem, psem):
    side = lax.axis_index('pp') // 4

    def tile(n, act):
        leg, b = n // 12, n % 12
        c = leg + side - 2 * leg * side
        at = n % 2

        def cols(j):
            return pl.ds(pl.multiple_of(j * DM, DM), DM)

        def three(left, right, out):
            if act == 'load':
                pltpu.make_async_copy(left, l_v.at[at], lsem.at[at]).start()
                pltpu.make_async_copy(right, r_v.at[at], rsem.at[at]).start()
            else:
                pltpu.make_async_copy(out_v.at[at], out, osem.at[at]).start()

        @pl.when(b < 3)
        def _():
            three(dt_hbm.at[leg, :, :, cols(b)], a_hbm.at[leg], gq_hbm.at[c, cols(b), :])

        @pl.when(b == 3)
        def _():
            three(o_hbm.at[leg], dh1_hbm.at[leg], go_hbm.at[c])

        @pl.when((b > 3) & (b < 8))
        def _():
            j = b - 4
            three(n2_hbm.at[leg], dz_hbm.at[leg, :, :, cols(j)], g1_hbm.at[c, :, cols(j)])

        @pl.when(b > 7)
        def _():
            j = b - 8
            three(u_hbm.at[leg, :, :, cols(j)], dh2_hbm.at[leg], g2_hbm.at[c, cols(j), :])

    tile(jnp.int32(0), 'load')

    def passing(act):
        for n, (src, dst) in enumerate(((y_in, y_hbm), (dx_in, dx_hbm))):
            into = pltpu.make_async_copy(src, pass_v.at[n], psem.at[n])
            out = pltpu.make_async_copy(pass_v.at[n], dst, psem.at[n])
            if act == 'in':
                into.start()
            elif act == 'out':
                into.wait()
                out.start()
            else:
                out.wait()

    passing('in')
    gbf_ref[...] = gbf_in[...]
    for c in range(2):
        for n in range(6):
            gvec_ref[c, n] = gvec_in[c, n:n + 1, :]
        for n in range(48):
            gbq_ref[c, n // 16, n % 16:n % 16 + 1, :] = gbq_in[c, :, n * 64:(n + 1) * 64]
    passing('out')

    def step(n, carry):
        at = n % 2

        @pl.when(n + 1 < N_TILES)
        def _():
            tile(n + 1, 'load')

        pltpu.make_async_copy(a_hbm.at[0], l_v.at[at], lsem.at[at]).wait()
        pltpu.make_async_copy(a_hbm.at[0], r_v.at[at], rsem.at[at]).wait()

        @pl.when(n > 1)
        def _():
            pltpu.make_async_copy(out_v.at[at], go_hbm.at[0], osem.at[at]).wait()

        for k in range(DM // STRIP):
            rows = slice(k * STRIP, (k + 1) * STRIP)
            acc = rounded(dot_nn(l_v[at, 0, :, rows].T, r_v[at, 0]))
            for m in range(1, MICRO):
                acc = acc + rounded(dot_nn(l_v[at, m, :, rows].T, r_v[at, m]))
            out_v[at, rows, :] = acc
        tile(n, 'store')
        return carry

    lax.fori_loop(0, N_TILES, step, 0)
    for at in range(2):
        pltpu.make_async_copy(out_v.at[at], go_hbm.at[0], osem.at[at]).wait()
    passing('done')


def weight_grads(*saved):
    hbm = pl.BlockSpec(memory_space=pltpu.HBM)
    vmem = pl.BlockSpec(memory_space=pltpu.VMEM)
    dma = pltpu.SemaphoreType.DMA
    return pl.pallas_call(
        wgrad_kernel,
        out_shape=tuple(jax.ShapeDtypeStruct((2,) + s, F32) for s in ((3 * DM, DM), (DM, DM), (DM, FF), (FF, DM)))
        + (jax.ShapeDtypeStruct((SEQ, DM), BF),) * 2
        + tuple(jax.ShapeDtypeStruct((2,) + s, F32) for s in ((3, 16, 64), (1, FF), (6, 1, DM))),
        in_specs=[hbm] * 10 + [vmem] * 3,
        out_specs=tuple([hbm] * 6 + [vmem] * 3),
        scratch_shapes=[
            pltpu.VMEM((2, MICRO, SEQ, DM), BF), pltpu.VMEM((2, MICRO, SEQ, DM), BF), pltpu.VMEM((2, DM, DM), F32),
            pltpu.VMEM((2, SEQ, DM), BF), dma((2,)), dma((2,)), dma((2,)), dma((2,)),
        ],
        compiler_params=pltpu.CompilerParams(vmem_limit_bytes=67000000),
        name="wgrad",
    )(*saved)


def solution(mesh):
    data_spec = P(('dp', 'pp'))
    weight_spec = P('pp')

    def per_device(x_loc, dy_loc, w_qkv, w_attn, w_fc, w_proj, b_qkv, b_fc, vec_d):
        wq = jnp.transpose(w_qkv, (0, 1, 2, 4, 5, 6, 3)).reshape(2, 3 * DM, DM)
        bq = b_qkv.reshape(2, 3, 16, 64)
        bf = b_fc.reshape(2, FF)
        vec = jnp.transpose(vec_d.reshape(2, 6, DM), (1, 0, 2))
        (y, dx, a, _, o, _, n2, _, u, _, dz, dt, dh1, dh2, gbq, gbf, gvec) = run_chain(
            x_loc.reshape(SEQ, DM), dy_loc.reshape(SEQ, DM), wq, w_attn.reshape(2, DM, DM), w_fc.reshape(2, DM, FF),
            w_proj.reshape(2, FF, DM), bq, bf, vec)
        gq, go, g1, g2, y, dx, gbq, gbf, gvec = weight_grads(dt, a, o, dh1, n2, dz, u, dh2, y, dx, gbq, gbf, gvec)
        gq = jnp.transpose(gq.reshape(1, 2, 1, 3, 16, 64, DM), (0, 1, 2, 6, 3, 4, 5))
        return (
            y.reshape(x_loc.shape), dx.reshape(x_loc.shape), gq, go.reshape(w_attn.shape), g1.reshape(w_fc.shape),
            g2.reshape(w_proj.shape), gbq.reshape(b_qkv.shape), gbf.reshape(b_fc.shape), gvec.reshape(vec_d.shape),
        )

    return jax.shard_map(per_device, mesh=mesh, in_specs=(data_spec, data_spec) + (weight_spec,) * 7,
                         out_specs=(data_spec, data_spec) + (data_spec,) * 7, check_vma=False)
```

```python
import jax
import jax.numpy as jnp
from jax import lax
from jax.experimental import pallas as pl
from jax.experimental.pallas import tpu as pltpu
from jax.sharding import PartitionSpec as P

EPSILON = 1e-5
SEQ = 128
DM = 1024
FF = 4096
MICRO = 8
OWN = MICRO // 2
PAIR = 2
WIDE = 256
HV, DV, OUT, YO = 0, 2 * MICRO, 4 * MICRO, 4 * MICRO + 2 * OWN
D1 = YO + OWN
N_SLOTS = D1 + 2 * OWN
FWD, BWD, FWD_FAR, BWD_FAR, NONE = 0, 1, 2, 3, 4
N_TASKS = 24
ORDER = (
    (0x2da2992582240c2040, 0xd93d12450fbcb26b9b),
    (0x2d9298266203902040, 0xdbe4f449143cb9bb1a),
    (0xb982ec2a4243202040, 0xfb6993d1245b41af19),
    (0x62eb242c3282241200, 0xf3eda6d136d2691650),
)
GELU_C = 0.7978845608028654
GELU_CA = GELU_C * 0.044715
NEG = -1e30
MESH = pl.DeviceIdType.MESH
BF = jnp.bfloat16
F32 = jnp.float32


def dot_nn(a, b):
    return lax.dot_general(a, b, (((1,), (0,)), ((), ())), preferred_element_type=F32)


def dot_nt(a, b):
    return lax.dot_general(a, b, (((1,), (1,)), ((), ())), preferred_element_type=F32)


def dot_tn(a, b):
    return lax.dot_general(a, b, (((0,), (0,)), ((), ())), preferred_element_type=F32)


def normalize(rows_f32):
    mean = jnp.mean(rows_f32, axis=-1, keepdims=True)
    centered = rows_f32 - mean
    var = jnp.mean(centered * centered, axis=-1, keepdims=True)
    rstd = lax.rsqrt(var + EPSILON)
    return centered * rstd, rstd


def rounded(v):
    return v.astype(BF).astype(F32)


def gelu_parts(z):
    zz = z * z
    th = jnp.tanh(z * (GELU_C + GELU_CA * zz))
    half = 0.5 + 0.5 * th
    return half, half + ((half * (1.0 - th)) * z) * (GELU_C + (3.0 * GELU_CA) * zz)


def strip(j):
    return slice(j * WIDE, (j + 1) * WIDE)


def inside_block(j):
    per = DM // WIDE
    return j // per, slice(j % per * WIDE, (j % per + 1) * WIDE)


def block(j):
    return slice(j * DM, (j + 1) * DM)


def chain_kernel(x_hbm, dy_hbm, wq_hbm, wo_hbm, w1_hbm, w2_hbm, bq_in, bf_in, vec_in,
                 y_hbm, dx_hbm, a_hbm, t_hbm, o_hbm, h1_hbm, n2_hbm, z_hbm, u_hbm, p_hbm,
                 dz_hbm, dt_hbm, dh1_hbm, dh2_hbm, gbq_ref, gbf_ref, gvec_ref,
                 bq_ref, bf_ref, vec_ref, wbuf, w1buf, buf, a_v, t_v, o_v, h1_v, n2_v, z_v, u_v, p_v, dt_v, dh1_v, do_v, gln_v, gln_far,
                 wsem, w1sem, fsem, bsem, lsem, recv_x, recv_dy, send_x, send_dy,
                 send_f, recv_f, send_b, recv_b, send_fm, recv_fm, send_bm, recv_bm, send_d1, recv_d1, send_g, recv_g, send_y, recv_y, send_dx, recv_dx):
    me = lax.axis_index('pp')
    dp = lax.axis_index('dp')
    side = me // 4
    pos = me + side * (7 - 2 * me)

    def place(q):
        return (dp, q + side * (7 - 2 * q))

    def copy_of(leg):
        return leg + side - 2 * leg * side

    codes = []
    for s in range(N_TASKS):
        row = [jnp.int32((ORDER[q][s // 12] >> (6 * (s % 12))) % 64) for q in range(4)]
        codes.append(jnp.where(pos == 0, row[0], jnp.where(pos == 1, row[1], jnp.where(pos == 2, row[2], row[3]))))

    def code_at(s):
        c = codes[0]
        for k in range(1, N_TASKS):
            c = jnp.where(s == k, codes[k], c)
        return c

    def parts(code):
        return code // 16, (code // 8) % 2, code % 8

    barrier = pltpu.get_barrier_semaphore()
    for k in range(1, 8):
        pl.semaphore_signal(barrier, inc=1, device_id=(dp, lax.rem(me + k, 8)), device_id_type=MESH)

    def block_copy(b, leg):
        c = copy_of(leg)
        if b < 3:
            src = wq_hbm.at[c, pl.ds(b * DM, DM), :]
        elif b == 3:
            src = wo_hbm.at[c]
        else:
            src = w2_hbm.at[c, pl.ds((b - 4) * DM, DM), :]
        return pltpu.make_async_copy(src, wbuf.at[b], wsem.at[b])

    def w1_copy(j, leg):
        return pltpu.make_async_copy(w1_hbm.at[copy_of(leg), :, pl.ds(j * DM, DM)], w1buf.at[leg, j], w1sem.at[leg * 4 + j])

    first_leg = parts(codes[0])[1]
    for b in range(4):
        block_copy(b, first_leg).start()
    for j in range(4):
        w1_copy(j, first_leg).start()
        block_copy(4 + j, first_leg).start()
    for j in range(4):
        w1_copy(j, 1 - first_leg).start()

    for c in range(2):
        bf_ref[c] = bf_in[c:c + 1, :].astype(F32)
        for n in range(6):
            vec_ref[c, n:n + 1, :] = vec_in[n, c:c + 1, :].astype(F32)
        for n in range(24):
            pair = bq_in[c, n // 8, 2 * (n % 8):2 * (n % 8) + 2, :].astype(F32)
            bq_ref[c, :, n * SEQ:(n + 1) * SEQ] = jnp.concatenate([pair[:1], pair[1:]], axis=1)
    gbq_ref[...] = jnp.zeros_like(gbq_ref)
    gbf_ref[...] = jnp.zeros_like(gbf_ref)
    gln_v[...] = jnp.zeros_like(gln_v)

    pl.semaphore_wait(barrier, 7)

    def spread(src, base, send, recv):
        dst = buf.at[base + pos]

        @pl.when(pos == 0)
        def _():
            pltpu.make_async_copy(src, dst, recv.at[0]).start()

        @pl.when(pos != 0)
        def _():
            pltpu.make_async_remote_copy(src_ref=src, dst_ref=dst, send_sem=send.at[0], recv_sem=recv.at[pos],
                                         device_id=place(0), device_id_type=MESH).start()

    spread(x_hbm, HV, send_x, recv_x)
    spread(dy_hbm, DV + MICRO, send_dy, recv_dy)

    def upward(kind, leg):
        return leg if kind == BWD else 1 - leg

    def hop(kind, leg, i):
        k, n = leg * MICRO + i, leg * OWN + i
        q = pos - 1 + 2 * upward(kind, leg)
        base, send, recv = (HV, send_f, recv_f) if kind == FWD else (DV, send_b, recv_b)
        return pltpu.make_async_remote_copy(src_ref=buf.at[OUT + n], dst_ref=buf.at[base + k], send_sem=send.at[n],
                                            recv_sem=recv.at[n], device_id=place(q), device_id_type=MESH)

    def mirror(kind, leg, i):
        k, n = leg * MICRO + i, leg * OWN + i
        base, send, recv = (HV, send_fm, recv_fm) if kind == FWD else (DV, send_bm, recv_bm)
        return pltpu.make_async_remote_copy(src_ref=buf.at[base + k], dst_ref=buf.at[base + k + OWN], send_sem=send.at[n],
                                            recv_sem=recv.at[n], device_id=(dp, 7 - me), device_id_type=MESH)

    def mirror_dh1(leg, i):
        n = leg * OWN + i
        return pltpu.make_async_remote_copy(src_ref=dh1_v.at[0], dst_ref=buf.at[D1 + n], send_sem=send_d1.at[0],
                                            recv_sem=recv_d1.at[n], device_id=(dp, 7 - me), device_id_type=MESH)

    def mirror_sums():
        return pltpu.make_async_remote_copy(src_ref=gln_v, dst_ref=gln_far, send_sem=send_g.at[0], recv_sem=recv_g.at[0],
                                            device_id=(dp, 7 - me), device_id_type=MESH)

    def hops_out(kind, leg):
        up = upward(kind, leg)
        return ((up == 1) & (pos < 3)) | ((up == 0) & (pos > 0))

    def hops_in(kind, leg):
        up = upward(kind, leg)
        return ((up == 1) & (pos > 0)) | ((up == 0) & (pos < 3))

    def f_saves(leg, i, n):
        pairs = ((a_v, a_hbm), (t_v, t_hbm), (o_v, o_hbm), (h1_v, h1_hbm), (n2_v, n2_hbm), (z_v, z_hbm), (u_v, u_hbm), (p_v, p_hbm))
        return [pltpu.make_async_copy(v.at[pl.ds(0, n)], h.at[leg, pl.ds(i, n)], fsem.at[m]) for m, (v, h) in enumerate(pairs)]

    def flush_forward(kind, leg, i, which):
        for n, of_kind in ((1, FWD), (PAIR, FWD_FAR)):
            @pl.when(kind == of_kind)
            def _():
                saves = f_saves(leg, i, n)
                for m in which:
                    if n == 1 or m != 3:
                        saves[m].wait()

    def b_saves(leg, i, n):
        own = pl.ds(0, n)
        dh1 = dh1_v if n == 1 else buf.at[pl.ds(D1 + leg * OWN + i - OWN, n)]
        pairs = ((u_v.at[pl.ds(PAIR - n, n)], dz_hbm), (dt_v.at[own], dt_hbm), (dh1, dh1_hbm), (buf.at[pl.ds(DV + leg * MICRO + i, n)], dh2_hbm))
        return [pltpu.make_async_copy(v, h.at[leg, pl.ds(i, n)], bsem.at[m]) for m, (v, h) in enumerate(pairs)]

    def b_loads(leg, i, n):
        pairs = ((z_hbm, z_v), (h1_hbm, h1_v), (t_hbm, t_v), (p_hbm, p_v))
        return [pltpu.make_async_copy(h.at[leg, pl.ds(i, n)], v.at[pl.ds(0, n)], lsem.at[m]) for m, (h, v) in enumerate(pairs)]

    def flush_backward(kind, leg, i, which):
        for n, of_kind in ((1, BWD), (PAIR, BWD_FAR)):
            @pl.when(kind == of_kind)
            def _():
                saves = b_saves(leg, i, n)
                for m in which:
                    saves[m].wait()

    def to_home(slot, i, dst, send, recv, act):
        src = buf.at[slot]

        @pl.when(i == 0)
        def _():
            if act == 'start':
                pltpu.make_async_copy(src, dst, recv).start()

        @pl.when((i > 0) & (i < OWN))
        def _():
            rc = pltpu.make_async_remote_copy(src_ref=src, dst_ref=dst, send_sem=send.at[i], recv_sem=recv,
                                              device_id=place(i), device_id_type=MESH)
            if act == 'start':
                rc.start()
            else:
                rc.wait_send()

    lane = lax.broadcasted_iota(jnp.int32, (1, SEQ), 1)
    low = jnp.where(lane < 64, 1.0, 0.0).astype(BF)
    high = jnp.where(lane < 64, 0.0, 1.0).astype(BF)
    q_idx = lax.broadcasted_iota(jnp.int32, (2 * SEQ, SEQ), 0) % SEQ
    k_idx = lax.broadcasted_iota(jnp.int32, (2 * SEQ, SEQ), 1)
    causal = q_idx >= k_idx

    def split_heads(v):
        return jnp.concatenate([v * low, v * high], axis=0)

    def side_by_side(v):
        return jnp.concatenate([v[:SEQ], v[SEQ:]], axis=1)

    def heads(ref, r, part):
        return [ref[r, :, part * DM + p * SEQ:part * DM + (p + 1) * SEQ] for p in range(8)]

    def probs(s):
        s = jnp.where(causal, s * 0.125, NEG)
        e = jnp.exp(s - jnp.max(s, axis=-1, keepdims=True))
        return e * (1.0 / jnp.sum(e, axis=-1, keepdims=True))

    def weights_for(leg, next_leg, fresh, moving):
        def need(*blocks):
            @pl.when(fresh)
            def _():
                for b in blocks:
                    block_copy(b, leg).wait()

        def release(*blocks):
            @pl.when(moving)
            def _():
                for b in blocks:
                    block_copy(b, next_leg).start()

        return need, release

    def flat(v):
        return v.reshape(v.shape[0] * v.shape[1], v.shape[2])

    def pieces(v):
        return v.reshape(v.shape[0] // SEQ, SEQ, v.shape[1])

    def forward_task(n, far, leg, i, before_kind, before_leg, before_i, need, release):
        c = copy_of(leg)
        k = leg * MICRO + i
        own = slice(0, n)

        if far:
            for r in range(n):
                mirror(FWD, leg, i - OWN + r).wait_recv()
        else:
            @pl.when((leg == 0) & (pos == 0))
            def _():
                pltpu.make_async_copy(x_hbm, buf.at[HV + i], recv_x.at[i]).wait()

            @pl.when(hops_in(FWD, leg))
            def _():
                hop(FWD, leg, i).wait_recv()

            mirror(FWD, leg, i).start()

        saves = f_saves(leg, i, n)
        need(0, 1, 2)
        xh, _ = normalize(flat(buf[pl.ds(HV + k, n)]).astype(F32))
        a_v[own] = pieces((xh * vec_ref[c, 0:1, :] + vec_ref[c, 1:2, :]).astype(BF))
        for j in range(3):
            t_v[own, :, block(j)] = pieces((dot_nt(flat(a_v[own]), wbuf[j]) + bq_ref[c, :, block(j)]).astype(BF))
        saves[0].start()
        saves[1].start()
        release(0, 1, 2)
        ss = [[dot_nt(split_heads(q), kk) for q, kk in zip(heads(t_v, r, 0), heads(t_v, r, 1))] for r in range(n)]
        ps = [[probs(sc) for sc in row] for row in ss]
        for r in range(n):
            for m, (p, v) in enumerate(zip(ps[r], heads(t_v, r, 2))):
                p_v[r, m] = p
                o_v[r, :, m * SEQ:(m + 1) * SEQ] = dot_nn(side_by_side(p.astype(BF)), split_heads(v)).astype(BF)
        saves[2].start()
        saves[7].start()
        need(3)
        h1 = flat(buf[pl.ds(HV + k, n)]).astype(F32) + dot_nn(flat(o_v[own]), wbuf[3]) + vec_ref[c, 2:3, :]
        h1_v[own] = pieces(h1.astype(BF))
        xh, _ = normalize(flat(h1_v[own]).astype(F32))
        n2_v[own] = pieces((xh * vec_ref[c, 3:4, :] + vec_ref[c, 4:5, :]).astype(BF))
        if not far:
            saves[3].start()
        saves[4].start()
        release(3)
        need(4, 5, 6, 7)

        @pl.when(i == 0)
        def _():
            for j in range(4):
                w1_copy(j, leg).wait()

        flush_forward(before_kind, before_leg, before_i, (5, 6))

        def hidden(j):
            b, cols = inside_block(j)
            z = dot_nn(flat(n2_v[own]), w1buf[leg, b, :, cols]) + bf_ref[c, :, strip(j)]
            half, slope = gelu_parts(z)
            u_v[own, :, strip(j)] = pieces((z * half).astype(BF))
            z_v[own, :, strip(j)] = pieces(z if far else slope)

        hidden(0)
        acc = jnp.zeros((n * SEQ, DM), F32)
        for j in range(FF // WIDE):
            if j < FF // WIDE - 1:
                hidden(j + 1)
            if not far:
                b, rows = inside_block(j)
                acc = acc + dot_nn(flat(u_v[own, :, strip(j)]), wbuf[4 + b, rows, :])
        if not far:
            h2 = (flat(h1_v[own]).astype(F32) + (acc + vec_ref[c, 5:6, :])).astype(BF)
            home = (leg == 1) & (pos == 0)
            inside = (leg == 0) & (pos == 3)
            buf[jnp.where(home, YO + i, jnp.where(inside, HV + MICRO + i, OUT + leg * OWN + i))] = h2

            @pl.when(hops_out(FWD, leg))
            def _():
                hop(FWD, leg, i).start()

            @pl.when(home)
            def _():
                to_home(YO + i, i, y_hbm, send_y, recv_y.at[0], 'start')

        saves[5].start()
        saves[6].start()
        release(4, 5, 6, 7)

    def backward_task(n, far, leg, i, before_kind, before_leg, before_i, next_kind, next_leg, next_i, need, release):
        c = copy_of(leg)
        k = leg * MICRO + i
        own, dz_at = slice(0, n), slice(PAIR - n, PAIR)
        loads = b_loads(leg, i, n)

        after_b = (before_kind == BWD) | (before_kind == BWD_FAR)

        inplace = (before_kind == FWD) & (before_leg == leg) & (before_i == i) & (not far)

        @pl.when(jnp.logical_not(inplace))
        def _():
            flush_forward(before_kind, before_leg, before_i, (5, 6))

        @pl.when(jnp.logical_not(after_b | inplace))
        def _():
            for m, ld in enumerate(loads):
                if m != 1 or not far:
                    ld.start()

        def arrived(*which):
            @pl.when(jnp.logical_not(inplace))
            def _():
                for m in which:
                    loads[m].wait()

        def prefetch(m):
            for next_n, of_kind in ((1, BWD), (PAIR, BWD_FAR)):
                if m != 1 or of_kind == BWD:
                    @pl.when(next_kind == of_kind)
                    def _():
                        b_loads(next_leg, next_i, next_n)[m].start()

        if far:
            for r in range(n):
                mirror(BWD, leg, i - OWN + r).wait_recv()
        else:
            @pl.when((leg == 1) & (pos == 0))
            def _():
                pltpu.make_async_copy(dy_hbm, buf.at[DV + k], recv_dy.at[i]).wait()

            @pl.when(hops_in(BWD, leg))
            def _():
                hop(BWD, leg, i).wait_recv()

            mirror(BWD, leg, i).start()

        def tally(ref, at, row, cols, v):
            ref[at, row:row + 1, cols] += rounded(jnp.sum(v, axis=0, keepdims=True))

        saves = b_saves(leg, i, n)
        saves[3].start()
        need(4, 5, 6, 7)
        if far:
            arrived(0)
        else:
            arrived(0, 1)
            second_norm = normalize(h1_v[0].astype(F32))
            first_norm = normalize(buf[HV + k].astype(F32))
            tally(gln_v, leg, 5, slice(0, DM), buf[DV + k].astype(F32))

        def norm_back(row, normalized, d_out):
            xh, rstd = normalized
            d_out = rounded(d_out)
            tally(gln_v, leg, row, every, d_out * xh)
            tally(gln_v, leg, row + 1, every, d_out)
            gx = d_out * vec_ref[c, row:row + 1, :]
            m1 = jnp.mean(gx, axis=-1, keepdims=True)
            m2 = jnp.mean(gx * xh, axis=-1, keepdims=True)
            return rounded(rstd * (gx - m1 - xh * m2))

        every = slice(0, DM)
        dh2 = flat(buf[pl.ds(DV + k, n)])

        def hidden(j):
            z = flat(z_v[own, :, block(j)])
            dz = rounded(dot_nt(dh2, wbuf[4 + j])) * (gelu_parts(z)[1] if far else z)
            for r in range(n):
                tally(gbf_ref, c, 0, block(j), dz[r * SEQ:(r + 1) * SEQ])
            u_v[dz_at, :, block(j)] = pieces(dz.astype(BF))

        hidden(0)
        dn2 = jnp.zeros((n * SEQ, DM), F32)
        for j in range(4):
            if j < 3:
                hidden(j + 1)
            if not far:
                dn2 = dn2 + dot_nt(flat(u_v[dz_at, :, block(j)]), w1buf[leg, j])
        saves[0].start()
        release(4, 5, 6, 7)
        prefetch(0)
        need(3)
        if far:
            for r in range(n):
                mirror_dh1(leg, i - OWN + r).wait_recv()
            dh1 = flat(buf[pl.ds(D1 + leg * OWN + i - OWN, n)])
        else:
            @pl.when((leg == 0) | (i > 0))
            def _():
                mirror_dh1(leg, i).wait_send()

            dh1_v[0] = (buf[DV + k].astype(F32) + norm_back(3, second_norm, dn2)).astype(BF)
            mirror_dh1(leg, i).start()
            dh1 = dh1_v[0]
            tally(gln_v, leg, 2, every, dh1.astype(F32))
        do_v[own] = pieces(dot_nt(dh1, wbuf[3]).astype(BF))
        saves[2].start()
        release(3)
        prefetch(1)
        need(0, 1, 2)
        arrived(2, 3)

        @pl.when(inplace)
        def _():
            flush_forward(before_kind, before_leg, before_i, (5, 6))

        flush_backward(before_kind, before_leg, before_i, (1,))
        if not far:
            @pl.when(hops_out(FWD, leg))
            def _():
                hop(FWD, leg, i).wait_send()

        def scores_back(r):
            dos = [split_heads(d) for d in heads(do_v, r, 0)]
            dps = [dot_nt(d, v) for d, v in zip(dos, heads(t_v, r, 2))]
            dss = []
            for m, dpv in enumerate(dps):
                p, dpv = p_v[r, m], rounded(dpv)
                dss.append((p * (dpv - jnp.sum(dpv * p, axis=-1, keepdims=True)) * 0.125).astype(BF))
            return dos, dss

        def heads_back(r, dos, dss):
            for m, (q, kk) in enumerate(zip(heads(t_v, r, 0), heads(t_v, r, 1))):
                lo = m * SEQ
                dt_v[r, :, lo:lo + SEQ] = dot_nn(side_by_side(dss[m]), split_heads(kk)).astype(BF)
                dt_v[r, :, DM + lo:DM + lo + SEQ] = dot_tn(dss[m], split_heads(q)).astype(BF)
                dt_v[r, :, 2 * DM + lo:2 * DM + lo + SEQ] = dot_tn(p_v[r, m].astype(BF), dos[m]).astype(BF)

        def input_back(r):
            da = jnp.zeros((SEQ, DM), F32)
            for j in range(3):
                dtj = dt_v[r, :, block(j)]
                tally(gbq_ref, c, 0, block(j), dtj.astype(F32))
                if not far:
                    da = da + dot_nn(dtj, wbuf[j])
            if not far:
                dh = dh1_v[r].astype(F32) + norm_back(0, first_norm, da)
                buf[jnp.where((leg == 1) & (pos == 3), DV + i, OUT + leg * OWN + i) + r] = dh.astype(BF)

        ahead = [scores_back(r) for r in range(n)]
        for r in range(n):
            heads_back(r, *ahead[r])
            input_back(r)

        if not far:
            @pl.when(hops_out(BWD, leg))
            def _():
                hop(BWD, leg, i).start()

            @pl.when((leg == 0) & (pos == 0))
            def _():
                to_home(OUT + i, i, dx_hbm, send_dx, recv_dx.at[0], 'start')

            @pl.when((leg == 0) & (i == OWN - 1))
            def _():
                mirror_sums().start()

        saves[1].start()
        prefetch(2)
        prefetch(3)
        release(0, 1, 2)

    def slot(s, carry):
        kind, leg, i = parts(code_at(s))
        before_kind, before_leg, before_i = parts(code_at(jnp.maximum(s - 1, 0)))
        next_kind, next_leg, next_i = parts(code_at(jnp.minimum(s + 1, N_TASKS - 1)))
        next_kind = jnp.where(s == N_TASKS - 1, NONE, next_kind)
        before_kind = jnp.where(s == 0, NONE, before_kind)
        need, release = weights_for(leg, next_leg, (s == 0) | (before_leg != leg), next_leg != leg)
        flush_forward(before_kind, before_leg, before_i, (0, 1, 2, 3, 4, 7))

        flush_backward(before_kind, before_leg, before_i, (0, 2, 3))
        for n, of_kind in ((1, FWD), (PAIR, FWD_FAR)):
            @pl.when(kind == of_kind)
            def _():
                flush_backward(before_kind, before_leg, before_i, (1,))
                forward_task(n, of_kind == FWD_FAR, leg, i, before_kind, before_leg, before_i, need, release)

        for n, of_kind in ((1, BWD), (PAIR, BWD_FAR)):
            @pl.when(kind == of_kind)
            def _():
                backward_task(n, of_kind == BWD_FAR, leg, i, before_kind, before_leg, before_i, next_kind, next_leg, next_i, need, release)

        return carry

    lax.fori_loop(0, N_TASKS, slot, 0)
    flush_backward(*parts(codes[N_TASKS - 1]), (0, 1, 2, 3))
    for leg in range(2):
        for i in range(OWN):
            mirror(FWD, leg, i).wait_send()
            mirror(BWD, leg, i).wait_send()

            @pl.when(hops_out(BWD, leg))
            def _():
                hop(BWD, leg, i).wait_send()

    @pl.when(pos == 0)
    def _():
        for i in range(OWN):
            to_home(YO + i, jnp.int32(i), y_hbm, send_y, recv_y.at[0], 'wait')
            to_home(OUT + i, jnp.int32(i), dx_hbm, send_dx, recv_dx.at[0], 'wait')

    @pl.when(pos != 0)
    def _():
        for src, send in ((x_hbm, send_x), (dy_hbm, send_dy)):
            pltpu.make_async_remote_copy(src_ref=src, dst_ref=buf.at[HV], send_sem=send.at[0], recv_sem=recv_x.at[0],
                                         device_id=place(0), device_id_type=MESH).wait_send()

    mirror_dh1(0, OWN - 1).wait_send()
    mirror_sums().wait()
    for leg in range(2):
        gvec_ref[copy_of(leg)] = gln_v[leg] + gln_far[leg]
    pltpu.make_async_copy(buf.at[YO], y_hbm, recv_y.at[0]).wait()
    pltpu.make_async_copy(buf.at[YO], dx_hbm, recv_dx.at[0]).wait()


def run_chain(x, dy, wq, wo, w1, w2, bq, bf, vec):
    hbm = pl.BlockSpec(memory_space=pltpu.HBM)
    vmem = pl.BlockSpec(memory_space=pltpu.VMEM)
    dma = pltpu.SemaphoreType.DMA

    def saved(n, ty=BF):
        return jax.ShapeDtypeStruct((2, MICRO, SEQ, n), ty)

    def paired(n, ty=BF):
        return pltpu.VMEM((PAIR, SEQ, n), ty)

    return pl.pallas_call(
        chain_kernel,
        out_shape=(
            jax.ShapeDtypeStruct((SEQ, DM), BF), jax.ShapeDtypeStruct((SEQ, DM), BF),
            saved(DM), saved(3 * DM), saved(DM), saved(DM), saved(DM), saved(FF, F32), saved(FF),
            jax.ShapeDtypeStruct((2, MICRO, 8, 2 * SEQ, SEQ), F32),
            saved(FF), saved(3 * DM), saved(DM), saved(DM),
            jax.ShapeDtypeStruct((2, 1, 3 * DM), F32), jax.ShapeDtypeStruct((2, 1, FF), F32), jax.ShapeDtypeStruct((2, 8, DM), F32),
        ),
        in_specs=[hbm] * 6 + [vmem] * 3,
        out_specs=tuple([hbm] * 14 + [vmem] * 3),
        scratch_shapes=[
            pltpu.VMEM((2, 1, 3 * DM), F32), pltpu.VMEM((2, 1, FF), F32), pltpu.VMEM((2, 8, DM), F32),
            pltpu.VMEM((8, DM, DM), BF),
            pltpu.VMEM((2, 4, DM, DM), BF),
            pltpu.VMEM((N_SLOTS, SEQ, DM), BF),
            paired(DM), paired(3 * DM), paired(DM), paired(DM), paired(DM), paired(FF, F32), paired(FF),
            pltpu.VMEM((PAIR, 8, 2 * SEQ, SEQ), F32), paired(3 * DM), pltpu.VMEM((1, SEQ, DM), BF), paired(DM),
            pltpu.VMEM((2, 8, DM), F32), pltpu.VMEM((2, 8, DM), F32),
            dma((8,)), dma((8,)), dma((8,)), dma((4,)), dma((4,)), dma((OWN,)), dma((OWN,)), dma((1,)), dma((1,)),
            *[dma((2 * OWN,))] * 8, dma((1,)), dma((2 * OWN,)), dma((1,)), dma((1,)),
            dma((OWN,)), dma((1,)), dma((OWN,)), dma((1,)),
        ],
        compiler_params=pltpu.CompilerParams(collective_id=0, has_side_effects=True, vmem_limit_bytes=67000000),
        name="chain",
    )(x, dy, wq, wo, w1, w2, bq, bf, vec)


N_TILES = 24
STRIP = 256


def wgrad_kernel(dt_hbm, a_hbm, o_hbm, dh1_hbm, n2_hbm, dz_hbm, u_hbm, dh2_hbm, y_in, dx_in, gbq_in, gbf_in, gvec_in,
                 gq_hbm, go_hbm, g1_hbm, g2_hbm, y_hbm, dx_hbm, gbq_ref, gbf_ref, gvec_ref, l_v, r_v, out_v, pass_v,
                 lsem, rsem, osem, psem):
    side = lax.axis_index('pp') // 4

    def tile(n, act):
        leg, b = n // 12, n % 12
        c = leg + side - 2 * leg * side
        at = n % 2

        def cols(j):
            return pl.ds(pl.multiple_of(j * DM, DM), DM)

        def three(left, right, out):
            if act == 'load':
                pltpu.make_async_copy(left, l_v.at[at], lsem.at[at]).start()
                pltpu.make_async_copy(right, r_v.at[at], rsem.at[at]).start()
            else:
                pltpu.make_async_copy(out_v.at[at], out, osem.at[at]).start()

        @pl.when(b < 3)
        def _():
            three(dt_hbm.at[leg, :, :, cols(b)], a_hbm.at[leg], gq_hbm.at[c, cols(b), :])

        @pl.when(b == 3)
        def _():
            three(o_hbm.at[leg], dh1_hbm.at[leg], go_hbm.at[c])

        @pl.when((b > 3) & (b < 8))
        def _():
            j = b - 4
            three(n2_hbm.at[leg], dz_hbm.at[leg, :, :, cols(j)], g1_hbm.at[c, :, cols(j)])

        @pl.when(b > 7)
        def _():
            j = b - 8
            three(u_hbm.at[leg, :, :, cols(j)], dh2_hbm.at[leg], g2_hbm.at[c, cols(j), :])

    tile(jnp.int32(0), 'load')

    def passing(act):
        for n, (src, dst) in enumerate(((y_in, y_hbm), (dx_in, dx_hbm))):
            into = pltpu.make_async_copy(src, pass_v.at[n], psem.at[n])
            out = pltpu.make_async_copy(pass_v.at[n], dst, psem.at[n])
            if act == 'in':
                into.start()
            elif act == 'out':
                into.wait()
                out.start()
            else:
                out.wait()

    passing('in')
    gbf_ref[...] = gbf_in[...]
    for c in range(2):
        for n in range(6):
            gvec_ref[c, n] = gvec_in[c, n:n + 1, :]
        for n in range(48):
            gbq_ref[c, n // 16, n % 16:n % 16 + 1, :] = gbq_in[c, :, n * 64:(n + 1) * 64]
    passing('out')

    def step(n, carry):
        at = n % 2

        @pl.when(n + 1 < N_TILES)
        def _():
            tile(n + 1, 'load')

        pltpu.make_async_copy(a_hbm.at[0], l_v.at[at], lsem.at[at]).wait()
        pltpu.make_async_copy(a_hbm.at[0], r_v.at[at], rsem.at[at]).wait()

        @pl.when(n > 1)
        def _():
            pltpu.make_async_copy(out_v.at[at], go_hbm.at[0], osem.at[at]).wait()

        for k in range(DM // STRIP):
            rows = slice(k * STRIP, (k + 1) * STRIP)
            acc = rounded(dot_nn(l_v[at, 0, :, rows].T, r_v[at, 0]))
            for m in range(1, MICRO):
                acc = acc + rounded(dot_nn(l_v[at, m, :, rows].T, r_v[at, m]))
            out_v[at, rows, :] = acc
        tile(n, 'store')
        return carry

    lax.fori_loop(0, N_TILES, step, 0)
    for at in range(2):
        pltpu.make_async_copy(out_v.at[at], go_hbm.at[0], osem.at[at]).wait()
    passing('done')


def weight_grads(*saved):
    hbm = pl.BlockSpec(memory_space=pltpu.HBM)
    vmem = pl.BlockSpec(memory_space=pltpu.VMEM)
    dma = pltpu.SemaphoreType.DMA
    return pl.pallas_call(
        wgrad_kernel,
        out_shape=tuple(jax.ShapeDtypeStruct((2,) + s, F32) for s in ((3 * DM, DM), (DM, DM), (DM, FF), (FF, DM)))
        + (jax.ShapeDtypeStruct((SEQ, DM), BF),) * 2
        + tuple(jax.ShapeDtypeStruct((2,) + s, F32) for s in ((3, 16, 64), (1, FF), (6, 1, DM))),
        in_specs=[hbm] * 10 + [vmem] * 3,
        out_specs=tuple([hbm] * 6 + [vmem] * 3),
        scratch_shapes=[
            pltpu.VMEM((2, MICRO, SEQ, DM), BF), pltpu.VMEM((2, MICRO, SEQ, DM), BF), pltpu.VMEM((2, DM, DM), F32),
            pltpu.VMEM((2, SEQ, DM), BF), dma((2,)), dma((2,)), dma((2,)), dma((2,)),
        ],
        compiler_params=pltpu.CompilerParams(vmem_limit_bytes=67000000),
        name="wgrad",
    )(*saved)


def solution(mesh):
    data_spec = P(('dp', 'pp'))
    weight_spec = P('pp')

    def per_device(x_loc, dy_loc, w_qkv, w_attn, w_fc, w_proj, b_qkv, b_fc, vec_d):
        wq = jnp.transpose(w_qkv, (0, 1, 2, 4, 5, 6, 3)).reshape(2, 3 * DM, DM)
        bq = b_qkv.reshape(2, 3, 16, 64)
        bf = b_fc.reshape(2, FF)
        vec = jnp.transpose(vec_d.reshape(2, 6, DM), (1, 0, 2))
        (y, dx, a, _, o, _, n2, _, u, _, dz, dt, dh1, dh2, gbq, gbf, gvec) = run_chain(
            x_loc.reshape(SEQ, DM), dy_loc.reshape(SEQ, DM), wq, w_attn.reshape(2, DM, DM), w_fc.reshape(2, DM, FF),
            w_proj.reshape(2, FF, DM), bq, bf, vec)
        gq, go, g1, g2, y, dx, gbq, gbf, gvec = weight_grads(dt, a, o, dh1, n2, dz, u, dh2, y, dx, gbq, gbf, gvec)
        gq = jnp.transpose(gq.reshape(1, 2, 1, 3, 16, 64, DM), (0, 1, 2, 6, 3, 4, 5))
        return (
            y.reshape(x_loc.shape), dx.reshape(x_loc.shape), gq, go.reshape(w_attn.shape), g1.reshape(w_fc.shape),
            g2.reshape(w_proj.shape), gbq.reshape(b_qkv.shape), gbf.reshape(b_fc.shape), gvec.reshape(vec_d.shape),
        )

    return jax.shard_map(per_device, mesh=mesh, in_specs=(data_spec, data_spec) + (weight_spec,) * 7,
                         out_specs=(data_spec, data_spec) + (data_spec,) * 7, check_vma=False)
```
